256 devices in a mesh: groups: 2 (over z), lat: 128 (over y, x, core).
Axes of the slice: x: 8, y: 8, z: 2, core: 2. Of those that a mesh axis runs over, the one named last changes fastest.
The devices are a block of a 8x8x16 slice.
Arguments:
- grid: bfloat16 [8192, 16, 8192], P('lat', 'groups'), parts along dimension 1, may hold values from -6 to 6
- cycle_weights: float32 [8192], P('lat'), may hold values from 0.1 to 1
- order_ids: int32 [38], replicated, may hold values from 0 to 4095, as said below
- leaf_weight: bfloat16 [8192, 38, 64], P('lat'), may hold values from -0.75 to 0.75
- transfer: bfloat16 [7, 128, 38, 64, 128], P(None, 'lat'), may hold values from -0.5 to 0.5
- degree_weight: bfloat16 [4096, 38, 64], P('lat'), may hold values from -0.75 to 0.75
Outputs:
- spectrum: float32 [4096, 38, 32], P('lat', None, 'groups'), parts along dimension 2
The draws below stay inside these ranges and needn't reach their ends.
There are 2 independent parts, one for each index of `groups`. The reference program is written for one: setup_inputs(seed, part) draws one part's arguments, and reference() takes and returns one part's arrays. A program takes and returns all parts, laid end to end along the dimension named above; an argument that names none is the same for every part. Nothing has to cross between parts.
Inputs may be any that keep to these rules, and one draw needn't show every extreme that they name: `order_ids`: the 38 entries are distinct orders.
All inputs are finite; a program needn't handle non-finite values.
Results may differ from the reference program's by a relative error of at most 0.0023.
Values may be sent and summed in bfloat16 or wider, within the bound.
No kernel may reach another device: no remote copies, remote signals or barrier semaphores. Data moves between devices by JAX's collectives and lax.ppermute only.
A program may use at most 64 MiB of HBM per device.

```python
import math
import jax
import jax.numpy as jnp
from jax import lax

FIELDS = 8
CYCLE_DEV = 64
NLON = 8192
DEGREES = 4096
ORDERS = 38
RANK = 64
CYCLES = 8192
LEVELS = 7
N_LAT = 128


def draw_order_ids(key, part):
    chosen = jax.random.permutation(key, DEGREES)[:ORDERS]
    return chosen.astype(jnp.int32)


def level_of(key, extent, pieces, smallest, largest):
    loudness, own = 1.0, jax.random.fold_in(key, 6)
    for dim, parts in pieces:
        steps = jnp.exp(jax.random.uniform(jax.random.fold_in(own, dim), (parts,), jnp.float32, smallest / len(pieces), largest / len(pieces)))
        loudness = loudness * jnp.repeat(steps, extent[dim] // parts).reshape([-1 if axis == dim else 1 for axis in range(len(extent))])
    return loudness


def scatter_about(key, extent, spread, most, cuts=(), dtype=jnp.bfloat16):
    factor_of = level_of(key, extent, cuts, -0.22, 0.18) if cuts else 1.0
    entries = jax.random.normal(key, extent, jnp.float32) * spread * factor_of
    return jnp.minimum(jnp.maximum(entries, -most), most).astype(dtype)


def setup_inputs(seed: int = 0, part: int = 0) -> dict:
    streams_of = jax.random.split(jax.random.key(seed), 7)
    part_splits = jax.random.split(jax.random.fold_in(streams_of[6], part), 7)
    return {
        "grid": scatter_about(part_splits[0], (CYCLES, FIELDS, NLON), 1.0, 6.0, ((0, 128),)),
        "cycle_weights": jnp.clip(jnp.exp(math.log(1.0) - 2.3025851 * jax.random.uniform(streams_of[1], (CYCLES,), jnp.float32) ** level_of(streams_of[1], (CYCLES,), ((0, 128),), -0.2, 0.2)), 0.1, 1.0),
        "order_ids": draw_order_ids(jax.random.fold_in(streams_of[6], 71), part),
        "leaf_weight": scatter_about(streams_of[3], (CYCLES, ORDERS, RANK), CYCLE_DEV ** -0.5, 0.75, ((0, 128),)),
        "transfer": scatter_about(streams_of[4], (LEVELS, N_LAT, ORDERS, RANK, 2 * RANK), (2 * RANK) ** -0.5, 0.5, ((1, 128),)),
        "degree_weight": scatter_about(streams_of[5], (DEGREES, ORDERS, RANK), RANK ** -0.5, 0.75, ((0, 128),)),
    }


def spectra(grid, cycle_weights, order_ids):
    cycles, fields, nlon = grid.shape
    count = order_ids.shape[0]
    longitude = lax.iota(jnp.int32, nlon)
    index = order_ids[:, None].astype(jnp.int32) * longitude[None, :] % nlon
    angle = index.astype(jnp.float32) * jnp.float32(2.0 * math.pi / nlon)
    table = jnp.concatenate([jnp.cos(angle), -jnp.sin(angle)], 0).astype(jnp.bfloat16)
    raw = jnp.dot(grid.reshape(cycles * fields, nlon), table.T, preferred_element_type=jnp.float32)
    raw = raw.reshape(cycles, fields, 2, count).transpose(0, 2, 1, 3).reshape(cycles, 2 * fields, count)
    return raw * (cycle_weights[:, None, None] / jnp.float32(math.sqrt(nlon)))

def reference(grid, cycle_weights, order_ids, leaf_weight, transfer, degree_weight):
    waves = spectra(grid, cycle_weights, order_ids)
    nodes = N_LAT
    width = waves.shape[1]
    blocks = waves.reshape(nodes, CYCLE_DEV, width, ORDERS)
    leaves = leaf_weight.astype(jnp.float32).reshape(nodes, CYCLE_DEV, ORDERS, RANK)
    current = jnp.einsum('nkor,nkqo->norq', leaves, blocks, precision=lax.Precision.HIGHEST)
    for level in range(LEVELS):
        span = 2 ** level
        groups = nodes // (2 * span)
        split = current.reshape(groups, 2, span, ORDERS, RANK, width)
        joined = jnp.concatenate([split[:, 0], split[:, 1]], axis=3)
        factors = transfer[level].astype(jnp.float32).reshape(groups, 2, span, ORDERS, RANK, 2 * RANK)
        current = jnp.einsum('gtpors,gposq->gtporq', factors, joined, precision=lax.Precision.HIGHEST)
        current = current.reshape(nodes, ORDERS, RANK, width)
    per_node = DEGREES // nodes
    finals = degree_weight.astype(jnp.float32).reshape(nodes, per_node, ORDERS, RANK)
    result = jnp.einsum('ndor,norq->ndoq', finals, current, precision=lax.Precision.HIGHEST)
    result = result.reshape(DEGREES, ORDERS, width)
    degree = lax.iota(jnp.int32, DEGREES)
    keep = degree[:, None] >= order_ids[None, :].astype(jnp.int32)
    return jnp.where(keep[:, :, None], result, jnp.float32(0.0))
```

```python
import math

import jax
import jax.numpy as jnp
from jax import lax
from jax.experimental import pallas as pl
from jax.experimental.pallas import tpu as pltpu
from jax.sharding import PartitionSpec as P

F32, BF16, I16, I32 = jnp.float32, jnp.bfloat16, jnp.int16, jnp.int32
LANES = 128
BLOCK = 8
CODE = 32000.0


def from_partner(block, axis, distance):
    count = lax.axis_size(axis)
    route = []
    for low in range(count):
        high = low | 1 << distance
        if high != low and high < count:
            route += [(low, high), (high, low)]
    return lax.ppermute(block, axis, route)


def lanes_of(shape):
    return lax.broadcasted_iota(I32, shape, len(shape) - 1)


def cos_sin(step, nlon):
    quarter, eighth = nlon // 4, nlon // 8
    moved = step + eighth
    quadrant = moved // quarter & 3
    x = ((moved & quarter - 1) - eighth).astype(F32) * F32(2.0 * math.pi / nlon)
    y = x * x
    c = 1.0 + y * (-0.5 + y * (1 / 24 + y * (-1 / 720 + y * (1 / 40320 - y / 3628800))))
    s = x * (1.0 + y * (-1 / 6 + y * (1 / 120 + y * (-1 / 5040 + y / 362880))))
    swap = quadrant & 1 == 1
    cos = jnp.where(swap, s, c)
    sin = jnp.where(swap, c, s)
    cos = jnp.where((quadrant == 1) | (quadrant == 2), -cos, cos)
    sin = jnp.where(quadrant >= 2, -sin, sin)
    return cos, sin


def split(value):
    high = value.astype(BF16)
    return high, (value - high.astype(F32)).astype(BF16)


def encode(values, send):
    rank = values[0].shape[0]
    peak = jnp.full((8, LANES), 1e-30, F32)
    for value in values:
        for row in range(0, rank, 8):
            peak = jnp.maximum(peak, jnp.abs(value[row : row + 8]))
    exponent = jnp.ceil(jnp.log2(peak))
    scale = jnp.exp2(-exponent) * CODE
    scale = jnp.concatenate([scale] * (rank // 8), 0)
    for g, value in enumerate(values):
        send[g * rank : (g + 1) * rank, :] = (value * scale).astype(I32).astype(I16)
    both = jnp.concatenate([exponent, exponent], 0)
    send[len(values) * rank :, :] = both.astype(I32).astype(I16)


def pick(product, rows):
    lane = lanes_of((rows, LANES)) % BLOCK
    chosen = jnp.zeros((rows, LANES), F32)
    for o in range(product.shape[0] // rows):
        chosen = jnp.where(lane == o, product[o * rows : (o + 1) * rows], chosen)
    return chosen


def analyse_kernel(ids_hbm, weights_hbm, leaf_hbm, grid_hbm, own_ref, send_ref,
                   ids, weights, leaf, grid, table, turned, raw, sems, grid_sems, *, fields, pieces):
    rows, nlon = grid.shape
    orders, cycles, rank = leaf.shape
    piece = nlon // pieces
    groups = pl.cdiv(orders, BLOCK)
    loads = []
    for i in range(pieces):
        cut = (slice(None), slice(i * piece, (i + 1) * piece))
        loads.append(pltpu.make_async_copy(grid_hbm.at[cut], grid.at[cut], grid_sems.at[i]))
    ids_load = pltpu.make_async_copy(ids_hbm, ids, sems.at[0])
    weights_load = pltpu.make_async_copy(weights_hbm, weights, sems.at[1])
    leaf_load = pltpu.make_async_copy(leaf_hbm, leaf, sems.at[2])
    ids_load.start()
    loads[0].start()
    loads[1].start()
    weights_load.start()
    leaf_load.start()
    for load in loads[2:]:
        load.start()
    half = 48
    ids_load.wait()
    row = lax.broadcasted_iota(I32, (half, LANES), 0)
    order = jnp.zeros((half, LANES), I32)
    for o in range(orders):
        order = jnp.where(row == o, ids[o], order)
    fine_c, fine_s = cos_sin(order * lanes_of((half, LANES)) & nlon - 1, nlon)
    coarse_c, coarse_s = cos_sin(order * (lanes_of((half, LANES)) * LANES) & nlon - 1, nlon)
    turn_c = coarse_c[:, piece // LANES : piece // LANES + 1] + jnp.zeros((half, LANES), F32)
    turn_s = coarse_s[:, piece // LANES : piece // LANES + 1] + jnp.zeros((half, LANES), F32)
    for a in range(piece // LANES):
        ca, sa = coarse_c[:, a : a + 1], coarse_s[:, a : a + 1]
        c, s = ca * fine_c - sa * fine_s, sa * fine_c + ca * fine_s
        for i in range(pieces):
            at = slice(i * piece + a * LANES, i * piece + (a + 1) * LANES)
            table[0:half, at] = c.astype(BF16)
            table[64 : 64 + half, at] = (-s).astype(BF16)
            if i + 1 < pieces:
                c, s = c * turn_c - s * turn_s, s * turn_c + c * turn_s
    weights_load.wait()
    leaf_load.wait()
    for o in range(orders):
        turned[o * rank : (o + 1) * rank, :] = jnp.concatenate([leaf[o], leaf[o]], 0).T
    weight = jnp.broadcast_to(weights[:, :], (LANES, cycles)).T * F32(1.0 / math.sqrt(nlon))
    for i in range(pieces):
        loads[i].wait()
        at = slice(i * piece, (i + 1) * piece)
        part = lax.dot_general(grid[:, at], table[:, at], (((1,), (1,)), ((), ())), preferred_element_type=F32)
        raw[:, :] = part if i == 0 else raw[:, :] + part
    moved = []
    for f in range(fields):
        value = raw[pl.ds(f, cycles, stride=fields), :] * weight
        moved.append(pltpu.roll(value, BLOCK * f, 1) if f else value)
    slot = lanes_of((cycles, LANES)) // BLOCK
    results = []
    for g in range(groups):
        here = slot - g & fields - 1
        waves = moved[0]
        for f in range(1, fields):
            waves = jnp.where(here == f, moved[f], waves)
        high, low = split(waves)
        count = min(BLOCK, orders - g * BLOCK)
        at = slice(g * BLOCK * rank, (g * BLOCK + count) * rank)
        product = jnp.dot(turned[at, :], jnp.concatenate([high, low], 0), preferred_element_type=F32)
        results.append(pick(product, rank))
    for g in range(groups):
        own_ref[g * rank : (g + 1) * rank, :] = results[g]
    encode(results, send_ref)


def join(own_ref, got_ref, joined, upper, groups, rank):
    exponent = got_ref[groups * rank :, :].astype(I32).astype(F32)[0:8]
    scale = jnp.exp2(exponent) * F32(1.0 / CODE)
    scale = jnp.concatenate([scale] * (rank // 8), 0)
    for g in range(groups):
        at = slice(g * rank, (g + 1) * rank)
        own = own_ref[at, :]
        other = got_ref[at, :].astype(I32).astype(F32) * scale
        lower_half = jnp.where(upper, other, own)
        upper_half = jnp.where(upper, own, other)
        low_high, low_low = split(lower_half)
        up_high, up_low = split(upper_half)
        joined[g, 0:rank, :] = low_high
        joined[g, rank : 2 * rank, :] = up_high
        joined[g, 2 * rank : 3 * rank, :] = low_low
        joined[g, 3 * rank : 4 * rank, :] = up_low


def merge(factors, joined, groups):
    orders, rank, wide = factors.shape
    results = []
    for g in range(groups):
        count = min(BLOCK, orders - g * BLOCK)
        left = factors[g * BLOCK : g * BLOCK + count].reshape(count * rank, wide)
        product = jnp.dot(jnp.concatenate([left, left], 1), joined[g], preferred_element_type=F32)
        results.append(pick(product, rank))
    return results


def level_kernel(own_ref, got_ref, factors, next_ref, send_ref, joined, *, level):
    orders, rank, _ = factors.shape
    groups = joined.shape[0]
    upper = (lax.axis_index("lat") >> level) & 1 == 1
    join(own_ref, got_ref, joined, upper, groups, rank)
    results = merge(factors, joined, groups)
    for g in range(groups):
        next_ref[g * rank : (g + 1) * rank, :] = results[g]
    encode(results, send_ref)


def last_kernel(ids, own_ref, got_ref, factors, degree_weight, out_ref, joined, *, level):
    orders, rank, _ = factors.shape
    groups = joined.shape[0]
    degrees = degree_weight.shape[1]
    slots = LANES // BLOCK
    position = lax.axis_index("lat")
    upper = (position >> level) & 1 == 1
    join(own_ref, got_ref, joined, upper, groups, rank)
    finals = merge(factors, joined, groups)
    lane = lanes_of((degrees, LANES))
    degree = position * degrees + lax.broadcasted_iota(I32, (degrees, LANES), 0)
    outs = []
    for g in range(groups):
        count = min(BLOCK, orders - g * BLOCK)
        left = degree_weight[g * BLOCK : g * BLOCK + count].reshape(count * degrees, rank)
        high, low = split(finals[g])
        product = jnp.dot(left, jnp.concatenate([high, low], 1), preferred_element_type=F32)
        value = pick(product[:, :LANES] + product[:, LANES:], degrees)
        order = jnp.zeros((degrees, LANES), I32)
        for o in range(count):
            order = jnp.where(lane % BLOCK == o, ids[g * BLOCK + o], order)
        outs.append(jnp.where(degree >= order, value, F32(0.0)))
    slot = lane // BLOCK
    for q in range(slots):
        value = outs[0]
        for g in range(1, groups):
            value = jnp.where(slot == (q + g) % slots, outs[g], value)
        value = pltpu.roll(value, (LANES - BLOCK * q) % LANES, 1) if q else value
        out_ref[pl.ds(q, degrees, stride=slots), :] = value[:, :orders]


def body(grid, cycle_weights, order_ids, leaf_weight, transfer, degree_weight):
    cycles, fields, nlon = grid.shape
    orders, rank = leaf_weight.shape[1:]
    levels = transfer.shape[0]
    degrees = degree_weight.shape[0]
    groups = -(-orders // BLOCK)
    pieces = 8
    leaf = leaf_weight.transpose(1, 0, 2)
    last = degree_weight.transpose(1, 0, 2)
    hbm = pl.BlockSpec(memory_space=pl.ANY)
    vmem = pl.BlockSpec(memory_space=pltpu.VMEM)
    smem = pl.BlockSpec(memory_space=pltpu.SMEM)
    own_type = jax.ShapeDtypeStruct((groups * rank, LANES), F32)
    send_type = jax.ShapeDtypeStruct((groups * rank + 16, LANES), I16)
    joined = pltpu.VMEM((groups, 4 * rank, LANES), BF16)
    own, send = pl.pallas_call(
        lambda *refs: analyse_kernel(*refs, fields=fields, pieces=pieces),
        out_shape=(own_type, send_type),
        in_specs=[hbm] * 4,
        out_specs=(vmem, vmem),
        scratch_shapes=[
            pltpu.SMEM((orders,), I32),
            pltpu.VMEM((1, cycles), F32),
            pltpu.VMEM((orders, cycles, rank), BF16),
            pltpu.VMEM((cycles * fields, nlon), BF16),
            pltpu.VMEM((LANES, nlon), BF16),
            pltpu.VMEM((orders * rank, 2 * cycles), BF16),
            pltpu.VMEM((cycles * fields, LANES), F32),
            pltpu.SemaphoreType.DMA((3,)),
            pltpu.SemaphoreType.DMA((pieces,)),
        ],
        name="analyse",
    )(order_ids, cycle_weights.reshape(1, cycles), leaf, grid.reshape(cycles * fields, nlon))
    for level in range(levels):
        got = from_partner(send, "lat", level)
        factors = transfer[level, 0]
        if level + 1 < levels:
            own, send = pl.pallas_call(
                lambda *refs, level=level: level_kernel(*refs, level=level),
                out_shape=(own_type, send_type),
                in_specs=[vmem, vmem, vmem],
                out_specs=(vmem, vmem),
                scratch_shapes=[joined],
                name=f"level{level}",
            )(own, got, factors)
        else:
            out = pl.pallas_call(
                lambda *refs: last_kernel(*refs, level=level),
                out_shape=jax.ShapeDtypeStruct((degrees * 2 * fields, orders), F32),
                in_specs=[smem, vmem, vmem, vmem, vmem],
                out_specs=vmem,
                scratch_shapes=[joined],
                name="last",
            )(order_ids, own, got, factors, last)
    return out.reshape(degrees, 2 * fields, orders).transpose(0, 2, 1)


def solution(mesh):
    return jax.shard_map(
        body,
        mesh=mesh,
        in_specs=(
            P("lat", "groups", None),
            P("lat"),
            P(),
            P("lat", None, None),
            P(None, "lat", None, None, None),
            P("lat", None, None),
        ),
        out_specs=P("lat", None, "groups"),
        check_vma=False,
    )
```

```python
import math

import jax
import jax.numpy as jnp
from jax import lax
from jax.experimental import pallas as pl
from jax.experimental.pallas import tpu as pltpu
from jax.sharding import PartitionSpec as P

F32, BF16, I16, I32 = jnp.float32, jnp.bfloat16, jnp.int16, jnp.int32
LANES = 128
BLOCK = 8
CODE = 32000.0


def from_partner(block, axis, distance):
    count = lax.axis_size(axis)
    route = []
    for low in range(count):
        high = low | 1 << distance
        if high != low and high < count:
            route += [(low, high), (high, low)]
    return lax.ppermute(block, axis, route)


def lanes_of(shape):
    return lax.broadcasted_iota(I32, shape, len(shape) - 1)


def cos_sin(step, nlon):
    quarter, eighth = nlon // 4, nlon // 8
    moved = step + eighth
    quadrant = moved // quarter & 3
    x = ((moved & quarter - 1) - eighth).astype(F32) * F32(2.0 * math.pi / nlon)
    y = x * x
    c = 1.0 + y * (-0.5 + y * (1 / 24 + y * (-1 / 720 + y * (1 / 40320 - y / 3628800))))
    s = x * (1.0 + y * (-1 / 6 + y * (1 / 120 + y * (-1 / 5040 + y / 362880))))
    swap = quadrant & 1 == 1
    cos = jnp.where(swap, s, c)
    sin = jnp.where(swap, c, s)
    cos = jnp.where((quadrant == 1) | (quadrant == 2), -cos, cos)
    sin = jnp.where(quadrant >= 2, -sin, sin)
    return cos, sin


def split(value):
    high = value.astype(BF16)
    return high, (value - high.astype(F32)).astype(BF16)


def encode(values, send):
    rank = values[0].shape[0]
    peak = jnp.full((8, LANES), 1e-30, F32)
    for value in values:
        for row in range(0, rank, 8):
            peak = jnp.maximum(peak, jnp.abs(value[row : row + 8]))
    exponent = jnp.ceil(jnp.log2(peak))
    scale = jnp.exp2(-exponent) * CODE
    scale = jnp.concatenate([scale] * (rank // 8), 0)
    for g, value in enumerate(values):
        send[g * rank : (g + 1) * rank, :] = (value * scale).astype(I32).astype(I16)
    both = jnp.concatenate([exponent, exponent], 0)
    send[len(values) * rank :, :] = both.astype(I32).astype(I16)


def pick(product, rows):
    lane = lanes_of((rows, LANES)) % BLOCK
    chosen = jnp.zeros((rows, LANES), F32)
    for o in range(product.shape[0] // rows):
        chosen = jnp.where(lane == o, product[o * rows : (o + 1) * rows], chosen)
    return chosen


def analyse_kernel(ids_hbm, weights_hbm, leaf_hbm, transfer_hbm, last_hbm, grid_hbm, own_ref, send_ref, factors_ref, last_ref,
                   ids, weights, leaf, grid, table, turned, raw, sems, grid_sems, *, fields, pieces):
    rows, nlon = grid.shape
    orders, cycles, rank = leaf.shape
    piece = nlon // pieces
    groups = pl.cdiv(orders, BLOCK)
    loads = []
    for i in range(pieces):
        cut = (slice(None), slice(i * piece, (i + 1) * piece))
        loads.append(pltpu.make_async_copy(grid_hbm.at[cut], grid.at[cut], grid_sems.at[i]))
    ids_load = pltpu.make_async_copy(ids_hbm, ids, sems.at[0])
    weights_load = pltpu.make_async_copy(weights_hbm, weights, sems.at[1])
    leaf_load = pltpu.make_async_copy(leaf_hbm, leaf, sems.at[2])
    factors_load = pltpu.make_async_copy(transfer_hbm, factors_ref, sems.at[3])
    last_load = pltpu.make_async_copy(last_hbm, last_ref, sems.at[4])
    ids_load.start()
    loads[0].start()
    loads[1].start()
    weights_load.start()
    leaf_load.start()
    for load in loads[2:]:
        load.start()
    factors_load.start()
    last_load.start()
    half = 48
    ids_load.wait()
    row = lax.broadcasted_iota(I32, (half, LANES), 0)
    order = jnp.zeros((half, LANES), I32)
    for o in range(orders):
        order = jnp.where(row == o, ids[o], order)
    fine_c, fine_s = cos_sin(order * lanes_of((half, LANES)) & nlon - 1, nlon)
    coarse_c, coarse_s = cos_sin(order * (lanes_of((half, LANES)) * LANES) & nlon - 1, nlon)
    turn_c = coarse_c[:, piece // LANES : piece // LANES + 1] + jnp.zeros((half, LANES), F32)
    turn_s = coarse_s[:, piece // LANES : piece // LANES + 1] + jnp.zeros((half, LANES), F32)
    for a in range(piece // LANES):
        ca, sa = coarse_c[:, a : a + 1], coarse_s[:, a : a + 1]
        c, s = ca * fine_c - sa * fine_s, sa * fine_c + ca * fine_s
        for i in range(pieces):
            at = slice(i * piece + a * LANES, i * piece + (a + 1) * LANES)
            table[0:half, at] = c.astype(BF16)
            table[64 : 64 + half, at] = (-s).astype(BF16)
            if i + 1 < pieces:
                c, s = c * turn_c - s * turn_s, s * turn_c + c * turn_s
    weights_load.wait()
    leaf_load.wait()
    for o in range(orders):
        turned[o * rank : (o + 1) * rank, :] = jnp.concatenate([leaf[o], leaf[o]], 0).T
    weight = jnp.broadcast_to(weights[:, :], (LANES, cycles)).T * F32(1.0 / math.sqrt(nlon))
    for i in range(pieces):
        loads[i].wait()
        at = slice(i * piece, (i + 1) * piece)
        part = lax.dot_general(grid[:, at], table[:, at], (((1,), (1,)), ((), ())), preferred_element_type=F32)
        raw[:, :] = part if i == 0 else raw[:, :] + part
    moved = []
    for f in range(fields):
        value = raw[pl.ds(f, cycles, stride=fields), :] * weight
        moved.append(pltpu.roll(value, BLOCK * f, 1) if f else value)
    slot = lanes_of((cycles, LANES)) // BLOCK
    results = []
    for g in range(groups):
        here = slot - g & fields - 1
        waves = moved[0]
        for f in range(1, fields):
            waves = jnp.where(here == f, moved[f], waves)
        high, low = split(waves)
        count = min(BLOCK, orders - g * BLOCK)
        at = slice(g * BLOCK * rank, (g * BLOCK + count) * rank)
        product = jnp.dot(turned[at, :], jnp.concatenate([high, low], 0), preferred_element_type=F32)
        results.append(pick(product, rank))
    for g in range(groups):
        own_ref[g * rank : (g + 1) * rank, :] = results[g]
    encode(results, send_ref)
    factors_load.wait()
    last_load.wait()


def join(own_ref, got_ref, joined, upper, groups, rank):
    exponent = got_ref[groups * rank :, :].astype(I32).astype(F32)[0:8]
    scale = jnp.exp2(exponent) * F32(1.0 / CODE)
    scale = jnp.concatenate([scale] * (rank // 8), 0)
    for g in range(groups):
        at = slice(g * rank, (g + 1) * rank)
        own = own_ref[at, :]
        other = got_ref[at, :].astype(I32).astype(F32) * scale
        lower_half = jnp.where(upper, other, own)
        upper_half = jnp.where(upper, own, other)
        low_high, low_low = split(lower_half)
        up_high, up_low = split(upper_half)
        joined[g, 0:rank, :] = low_high
        joined[g, rank : 2 * rank, :] = up_high
        joined[g, 2 * rank : 3 * rank, :] = low_low
        joined[g, 3 * rank : 4 * rank, :] = up_low


def merge(factors, joined, groups):
    orders, rank, wide = factors.shape
    results = []
    for g in range(groups):
        count = min(BLOCK, orders - g * BLOCK)
        left = factors[g * BLOCK : g * BLOCK + count].reshape(count * rank, wide)
        product = jnp.dot(jnp.concatenate([left, left], 1), joined[g], preferred_element_type=F32)
        results.append(pick(product, rank))
    return results


def level_kernel(own_ref, got_ref, factors_ref, next_ref, send_ref, joined, *, level):
    factors = factors_ref.at[level]
    orders, rank, _ = factors.shape
    groups = joined.shape[0]
    upper = (lax.axis_index("lat") >> level) & 1 == 1
    join(own_ref, got_ref, joined, upper, groups, rank)
    results = merge(factors, joined, groups)
    for g in range(groups):
        next_ref[g * rank : (g + 1) * rank, :] = results[g]
    encode(results, send_ref)


def last_kernel(ids, own_ref, got_ref, factors_ref, degree_weight, out_ref, joined, *, level):
    factors = factors_ref.at[level]
    orders, rank, _ = factors.shape
    groups = joined.shape[0]
    degrees = degree_weight.shape[1]
    slots = LANES // BLOCK
    position = lax.axis_index("lat")
    upper = (position >> level) & 1 == 1
    join(own_ref, got_ref, joined, upper, groups, rank)
    finals = merge(factors, joined, groups)
    lane = lanes_of((degrees, LANES))
    degree = position * degrees + lax.broadcasted_iota(I32, (degrees, LANES), 0)
    outs = []
    for g in range(groups):
        count = min(BLOCK, orders - g * BLOCK)
        left = degree_weight[g * BLOCK : g * BLOCK + count].reshape(count * degrees, rank)
        high, low = split(finals[g])
        product = jnp.dot(left, jnp.concatenate([high, low], 1), preferred_element_type=F32)
        value = pick(product[:, :LANES] + product[:, LANES:], degrees)
        order = jnp.zeros((degrees, LANES), I32)
        for o in range(count):
            order = jnp.where(lane % BLOCK == o, ids[g * BLOCK + o], order)
        outs.append(jnp.where(degree >= order, value, F32(0.0)))
    slot = lane // BLOCK
    for q in range(slots):
        value = outs[0]
        for g in range(1, groups):
            value = jnp.where(slot == (q + g) % slots, outs[g], value)
        value = pltpu.roll(value, (LANES - BLOCK * q) % LANES, 1) if q else value
        out_ref[pl.ds(q, degrees, stride=slots), :] = value[:, :orders]


def in_vmem(value):
    return pltpu.with_memory_space_constraint(value, pltpu.VMEM)


def in_hbm(value):
    return pltpu.with_memory_space_constraint(value, pltpu.HBM)


def body(grid, cycle_weights, order_ids, leaf_weight, transfer, degree_weight):
    cycles, fields, nlon = grid.shape
    orders, rank = leaf_weight.shape[1:]
    levels = transfer.shape[0]
    degrees = degree_weight.shape[0]
    groups = -(-orders // BLOCK)
    pieces = 8
    leaf = leaf_weight.transpose(1, 0, 2)
    last = degree_weight.transpose(1, 0, 2)
    hbm = pl.BlockSpec(memory_space=pltpu.HBM)
    vmem = pl.BlockSpec(memory_space=pltpu.VMEM)
    smem = pl.BlockSpec(memory_space=pltpu.SMEM)
    own_type = pltpu.VMEM((groups * rank, LANES), F32)
    send_type = pltpu.VMEM((groups * rank + 16, LANES), I16)
    joined = pltpu.VMEM((groups, 4 * rank, LANES), BF16)
    own, send, factors, last = pl.pallas_call(
        lambda *refs: analyse_kernel(*refs, fields=fields, pieces=pieces),
        out_shape=(own_type, send_type, pltpu.VMEM(transfer.shape[:1] + transfer.shape[2:], BF16), pltpu.VMEM(last.shape, BF16)),
        in_specs=[hbm] * 6,
        out_specs=(vmem,) * 4,
        scratch_shapes=[
            pltpu.SMEM((orders,), I32),
            pltpu.VMEM((1, cycles), F32),
            pltpu.VMEM((orders, cycles, rank), BF16),
            pltpu.VMEM((cycles * fields, nlon), BF16),
            pltpu.VMEM((LANES, nlon), BF16),
            pltpu.VMEM((orders * rank, 2 * cycles), BF16),
            pltpu.VMEM((cycles * fields, LANES), F32),
            pltpu.SemaphoreType.DMA((5,)),
            pltpu.SemaphoreType.DMA((pieces,)),
        ],
        compiler_params=pltpu.CompilerParams(vmem_limit_bytes=32 * 2**20),
        name="analyse",
    )(*map(in_hbm, (order_ids, cycle_weights.reshape(1, cycles), leaf, transfer[:, 0], last, grid.reshape(cycles * fields, nlon))))
    own, send, factors, last = map(in_vmem, (own, send, factors, last))
    for level in range(levels):
        got = in_vmem(from_partner(send, "lat", level))
        if level + 1 < levels:
            own, send = pl.pallas_call(
                lambda *refs, level=level: level_kernel(*refs, level=level),
                out_shape=(own_type, send_type),
                in_specs=[vmem, vmem, vmem],
                out_specs=(vmem, vmem),
                scratch_shapes=[joined],
                compiler_params=pltpu.CompilerParams(vmem_limit_bytes=16 * 2**20),
                name=f"level{level}",
            )(own, got, factors)
            own, send = in_vmem(own), in_vmem(send)
        else:
            out = pl.pallas_call(
                lambda *refs: last_kernel(*refs, level=level),
                out_shape=jax.ShapeDtypeStruct((degrees * 2 * fields, orders), F32),
                in_specs=[smem, vmem, vmem, vmem, vmem],
                out_specs=vmem,
                scratch_shapes=[joined],
                compiler_params=pltpu.CompilerParams(vmem_limit_bytes=16 * 2**20),
                name="last",
            )(order_ids, own, got, factors, last)
    return out.reshape(degrees, 2 * fields, orders).transpose(0, 2, 1)


def solution(mesh):
    return jax.shard_map(
        body,
        mesh=mesh,
        in_specs=(
            P("lat", "groups", None),
            P("lat"),
            P(),
            P("lat", None, None),
            P(None, "lat", None, None, None),
            P("lat", None, None),
        ),
        out_specs=P("lat", None, "groups"),
        check_vma=False,
    )
```

```python
import math

import jax
import jax.numpy as jnp
from jax import lax
from jax.experimental import pallas as pl
from jax.experimental.pallas import tpu as pltpu
from jax.sharding import PartitionSpec as P

F32, BF16, I16, I32 = jnp.float32, jnp.bfloat16, jnp.int16, jnp.int32
LANES = 128
BLOCK = 8
CODE = 32000.0


def from_partner(block, axis, distance):
    count = lax.axis_size(axis)
    route = []
    for low in range(count):
        high = low | 1 << distance
        if high != low and high < count:
            route += [(low, high), (high, low)]
    return lax.ppermute(block, axis, route)


def lanes_of(shape):
    return lax.broadcasted_iota(I32, shape, len(shape) - 1)


def cos_sin(step, nlon):
    quarter, eighth = nlon // 4, nlon // 8
    moved = step + eighth
    quadrant = moved // quarter & 3
    x = ((moved & quarter - 1) - eighth).astype(F32) * F32(2.0 * math.pi / nlon)
    y = x * x
    c = 1.0 + y * (-0.5 + y * (1 / 24 + y * (-1 / 720 + y * (1 / 40320 - y / 3628800))))
    s = x * (1.0 + y * (-1 / 6 + y * (1 / 120 + y * (-1 / 5040 + y / 362880))))
    swap = quadrant & 1 == 1
    cos = jnp.where(swap, s, c)
    sin = jnp.where(swap, c, s)
    cos = jnp.where((quadrant == 1) | (quadrant == 2), -cos, cos)
    sin = jnp.where(quadrant >= 2, -sin, sin)
    return cos, sin


def split(value):
    high = value.astype(BF16)
    return high, (value - high.astype(F32)).astype(BF16)


def encode(values, send):
    rank = values[0].shape[0]
    peak = jnp.full((8, LANES), 1e-30, F32)
    for value in values:
        for row in range(0, rank, 8):
            peak = jnp.maximum(peak, jnp.abs(value[row : row + 8]))
    exponent = jnp.ceil(jnp.log2(peak))
    scale = jnp.exp2(-exponent) * CODE
    scale = jnp.concatenate([scale] * (rank // 8), 0)
    for g, value in enumerate(values):
        send[g * rank : (g + 1) * rank, :] = (value * scale).astype(I32).astype(I16)
    send[len(values) * rank :, :] = exponent.astype(I32).astype(I16)


def pick(product, rows):
    lane = lanes_of((rows, LANES)) % BLOCK
    chosen = jnp.zeros((rows, LANES), F32)
    for o in range(product.shape[0] // rows):
        chosen = jnp.where(lane == o, product[o * rows : (o + 1) * rows], chosen)
    return chosen


def analyse_kernel(ids_hbm, weights_hbm, leaf_hbm, transfer_hbm, grid_hbm, own_ref, send_ref, first_ref,
                   ids, weights, leaf, grid, table, turned, raw, wave_c, wave_s, sems, grid_sems, *, fields, pieces, turn):
    rows, nlon = grid.shape
    orders, cycles, rank = leaf.shape
    piece = nlon // pieces
    groups = pl.cdiv(orders, BLOCK)

    def load_of(i):
        cut = (slice(None), pl.ds(pl.multiple_of(i * piece, piece), piece))
        return pltpu.make_async_copy(grid_hbm.at[cut], grid.at[cut], grid_sems.at[i])

    loads = [load_of(i) for i in range(pieces)]
    ids_load = pltpu.make_async_copy(ids_hbm, ids, sems.at[0])
    weights_load = pltpu.make_async_copy(weights_hbm, weights, sems.at[1])
    leaf_load = pltpu.make_async_copy(leaf_hbm, leaf, sems.at[2])
    first_load = pltpu.make_async_copy(transfer_hbm.at[0], first_ref, sems.at[3])
    ids_load.start()
    weights_load.start()
    leaf_load.start()
    for load in loads:
        load.start()
    first_load.start()
    half = 48
    ids_load.wait()
    row = lax.broadcasted_iota(I32, (half, LANES), 0)
    order = jnp.zeros((half, LANES), I32)
    for o in range(orders):
        order = jnp.where(row == o, ids[o], order)
    fine_c, fine_s = cos_sin(order * lanes_of((half, LANES)) & nlon - 1, nlon)
    coarse_c, coarse_s = cos_sin(order * (lanes_of((half, LANES)) * LANES) & nlon - 1, nlon)
    turn_c = coarse_c[:, turn // LANES : turn // LANES + 1] + jnp.zeros((half, LANES), F32)
    turn_s = coarse_s[:, turn // LANES : turn // LANES + 1] + jnp.zeros((half, LANES), F32)
    for a in range(turn // LANES):
        ca, sa = coarse_c[:, a : a + 1], coarse_s[:, a : a + 1]
        at = slice(a * LANES, (a + 1) * LANES)
        wave_c[:, at], wave_s[:, at] = ca * fine_c - sa * fine_s, sa * fine_c + ca * fine_s

    def fill(i, carry):
        for a in range(turn // LANES):
            at = slice(a * LANES, (a + 1) * LANES)
            to = pl.ds(pl.multiple_of(i * turn + a * LANES, LANES), LANES)
            c, s = wave_c[:, at], wave_s[:, at]
            table[0:half, to] = c.astype(BF16)
            table[64 : 64 + half, to] = (-s).astype(BF16)
            wave_c[:, at], wave_s[:, at] = c * turn_c - s * turn_s, s * turn_c + c * turn_s
        return carry

    lax.fori_loop(0, nlon // turn, fill, 0)
    weights_load.wait()
    leaf_load.wait()
    raw[:, :] = jnp.zeros(raw.shape, F32)
    share = pl.cdiv(orders, pieces)

    def multiply(i, carry):
        load_of(i).wait()
        at = pl.ds(pl.multiple_of(i * piece, piece), piece)
        raw[:, :] += lax.dot_general(grid[:, at], table[:, at], (((1,), (1,)), ((), ())), preferred_element_type=F32)
        begin = jnp.minimum(i * share, orders - share)
        for u in range(share):
            o = begin + u
            turned[pl.ds(pl.multiple_of(o * rank, rank), rank), :] = jnp.concatenate([leaf[o], leaf[o]], 0).T
        return carry

    lax.fori_loop(0, pieces, multiply, 0)
    weight = jnp.broadcast_to(weights[:, :], (LANES, cycles)).T * F32(1.0 / math.sqrt(nlon))
    moved = []
    for f in range(fields):
        value = raw[pl.ds(f, cycles, stride=fields), :] * weight
        moved.append(pltpu.roll(value, BLOCK * f, 1) if f else value)
    slot = lanes_of((cycles, LANES)) // BLOCK
    results = []
    for g in range(groups):
        here = slot - g & fields - 1
        waves = moved[0]
        for f in range(1, fields):
            waves = jnp.where(here == f, moved[f], waves)
        high, low = split(waves)
        count = min(BLOCK, orders - g * BLOCK)
        at = slice(g * BLOCK * rank, (g * BLOCK + count) * rank)
        product = jnp.dot(turned[at, :], jnp.concatenate([high, low], 0), preferred_element_type=F32)
        results.append(pick(product, rank))
    for g in range(groups):
        own_ref[g * rank : (g + 1) * rank, :] = results[g]
    encode(results, send_ref)
    first_load.wait()


def join(own_ref, got_ref, joined, upper, groups, rank):
    exponent = got_ref[groups * rank :, :].astype(I32).astype(F32)
    scale = jnp.exp2(exponent) * F32(1.0 / CODE)
    scale = jnp.concatenate([scale] * (rank // 8), 0)
    for g in range(groups):
        at = slice(g * rank, (g + 1) * rank)
        own = own_ref[at, :]
        other = got_ref[at, :].astype(I32).astype(F32) * scale
        lower_half = jnp.where(upper, other, own)
        upper_half = jnp.where(upper, own, other)
        low_high, low_low = split(lower_half)
        up_high, up_low = split(upper_half)
        joined[g, 0:rank, :] = low_high
        joined[g, rank : 2 * rank, :] = up_high
        joined[g, 2 * rank : 3 * rank, :] = low_low
        joined[g, 3 * rank : 4 * rank, :] = up_low


def merge(factors, joined, groups):
    orders, rank, wide = factors.shape
    results = []
    for g in range(groups):
        count = min(BLOCK, orders - g * BLOCK)
        left = factors[g * BLOCK : g * BLOCK + count].reshape(count * rank, wide)
        product = jnp.dot(jnp.concatenate([left, left], 1), joined[g], preferred_element_type=F32)
        results.append(pick(product, rank))
    return results


def level_kernel(own_ref, got_ref, factors_ref, next_ref, send_ref, joined, *, level):
    factors = factors_ref.at[level - 1] if level else factors_ref
    orders, rank, _ = factors.shape
    groups = joined.shape[0]
    upper = (lax.axis_index("lat") >> level) & 1 == 1
    join(own_ref, got_ref, joined, upper, groups, rank)
    results = merge(factors, joined, groups)
    for g in range(groups):
        next_ref[g * rank : (g + 1) * rank, :] = results[g]
    encode(results, send_ref)


def fetch_kernel(after_ref, ids_hbm, transfer_hbm, last_hbm, factors_ref, last_ref, lanes_ref, ids, sems):
    del after_ref
    ids_load = pltpu.make_async_copy(ids_hbm, ids, sems.at[0])
    factors_load = pltpu.make_async_copy(transfer_hbm.at[1:], factors_ref, sems.at[1])
    last_load = pltpu.make_async_copy(last_hbm, last_ref, sems.at[2])
    ids_load.start()
    factors_load.start()
    last_load.start()
    ids_load.wait()
    lane = lanes_of((8, LANES)) % BLOCK
    for g in range(lanes_ref.shape[0]):
        order = jnp.zeros((8, LANES), I32)
        for o in range(min(BLOCK, ids.shape[0] - g * BLOCK)):
            order = jnp.where(lane == o, ids[g * BLOCK + o], order)
        lanes_ref[g] = order
    factors_load.wait()
    last_load.wait()


def last_kernel(lanes_ref, own_ref, got_ref, factors_ref, degree_weight, out_ref, joined, *, level):
    factors = factors_ref.at[level - 1]
    orders, rank, _ = factors.shape
    groups = joined.shape[0]
    degrees = degree_weight.shape[1]
    slots = LANES // BLOCK
    position = lax.axis_index("lat")
    upper = (position >> level) & 1 == 1
    join(own_ref, got_ref, joined, upper, groups, rank)
    finals = merge(factors, joined, groups)
    lane = lanes_of((degrees, LANES))
    degree = position * degrees + lax.broadcasted_iota(I32, (degrees, LANES), 0)
    outs = []
    for g in range(groups):
        count = min(BLOCK, orders - g * BLOCK)
        left = degree_weight[g * BLOCK : g * BLOCK + count].reshape(count * degrees, rank)
        high, low = split(finals[g])
        product = jnp.dot(left, jnp.concatenate([high, low], 1), preferred_element_type=F32)
        value = pick(product[:, :LANES] + product[:, LANES:], degrees)
        order = jnp.concatenate([lanes_ref[g]] * (degrees // 8), 0)
        outs.append(jnp.where(degree >= order, value, F32(0.0)))
    slot = lane // BLOCK
    for q in range(slots):
        value = outs[0]
        for g in range(1, groups):
            value = jnp.where(slot == (q + g) % slots, outs[g], value)
        value = pltpu.roll(value, (LANES - BLOCK * q) % LANES, 1) if q else value
        out_ref[pl.ds(q, degrees, stride=slots), :] = value[:, :orders]


def in_vmem(value):
    return pltpu.with_memory_space_constraint(value, pltpu.VMEM)


def in_hbm(value):
    return pltpu.with_memory_space_constraint(value, pltpu.HBM)


def body(grid, cycle_weights, order_ids, leaf_weight, transfer, degree_weight):
    cycles, fields, nlon = grid.shape
    orders, rank = leaf_weight.shape[1:]
    levels = transfer.shape[0]
    degrees = degree_weight.shape[0]
    groups = -(-orders // BLOCK)
    pieces = 2
    leaf = leaf_weight.transpose(1, 0, 2)
    last = degree_weight.transpose(1, 0, 2)
    hbm = pl.BlockSpec(memory_space=pltpu.HBM)
    vmem = pl.BlockSpec(memory_space=pltpu.VMEM)
    own_type = pltpu.VMEM((groups * rank, LANES), F32)
    send_type = pltpu.VMEM((groups * rank + 8, LANES), I16)
    joined = pltpu.VMEM((groups, 4 * rank, LANES), BF16)
    own, send, first = pl.pallas_call(
        lambda *refs: analyse_kernel(*refs, fields=fields, pieces=pieces, turn=1024),
        out_shape=(own_type, send_type, pltpu.VMEM(transfer.shape[2:], BF16)),
        in_specs=[hbm] * 5,
        out_specs=(vmem,) * 3,
        scratch_shapes=[
            pltpu.SMEM((orders,), I32),
            pltpu.VMEM((1, cycles), F32),
            pltpu.VMEM((orders, cycles, rank), BF16),
            pltpu.VMEM((cycles * fields, nlon), BF16),
            pltpu.VMEM((LANES, nlon), BF16),
            pltpu.VMEM((orders * rank, 2 * cycles), BF16),
            pltpu.VMEM((cycles * fields, LANES), F32),
            pltpu.VMEM((48, 1024), F32),
            pltpu.VMEM((48, 1024), F32),
            pltpu.SemaphoreType.DMA((4,)),
            pltpu.SemaphoreType.DMA((pieces,)),
        ],
        compiler_params=pltpu.CompilerParams(vmem_limit_bytes=32 * 2**20),
        name="analyse",
    )(*map(in_hbm, (order_ids, cycle_weights.reshape(1, cycles), leaf, transfer[:, 0], grid.reshape(cycles * fields, nlon))))
    own, send, first = map(in_vmem, (own, send, first))
    for level in range(levels):
        got = in_vmem(from_partner(send, "lat", level))
        if level + 1 < levels:
            own, send = pl.pallas_call(
                lambda *refs, level=level: level_kernel(*refs, level=level),
                out_shape=(own_type, send_type),
                in_specs=[vmem, vmem, vmem],
                out_specs=(vmem, vmem),
                scratch_shapes=[joined],
                compiler_params=pltpu.CompilerParams(vmem_limit_bytes=16 * 2**20),
                name=f"level{level}",
            )(own, got, factors if level else first)
            own, send = in_vmem(own), in_vmem(send)
            if not level:
                factors, last, order_lanes = map(in_vmem, pl.pallas_call(
                    fetch_kernel,
                    out_shape=(
                        pltpu.VMEM((levels - 1,) + transfer.shape[2:], BF16),
                        pltpu.VMEM(last.shape, BF16),
                        pltpu.VMEM((groups, 8, LANES), I32),
                    ),
                    in_specs=[vmem] + [hbm] * 3,
                    out_specs=(vmem,) * 3,
                    scratch_shapes=[pltpu.SMEM((orders,), I32), pltpu.SemaphoreType.DMA((3,))],
                    compiler_params=pltpu.CompilerParams(vmem_limit_bytes=16 * 2**20),
                    name="fetch",
                )(own, *map(in_hbm, (order_ids, transfer[:, 0], last))))
        else:
            out = pl.pallas_call(
                lambda *refs: last_kernel(*refs, level=level),
                out_shape=jax.ShapeDtypeStruct((degrees * 2 * fields, orders), F32),
                in_specs=[vmem] * 5,
                out_specs=vmem,
                scratch_shapes=[joined],
                compiler_params=pltpu.CompilerParams(vmem_limit_bytes=16 * 2**20),
                name="last",
            )(order_lanes, own, got, factors, last)
    return out.reshape(degrees, 2 * fields, orders).transpose(0, 2, 1)


def solution(mesh):
    return jax.shard_map(
        body,
        mesh=mesh,
        in_specs=(
            P("lat", "groups", None),
            P("lat"),
            P(),
            P("lat", None, None),
            P(None, "lat", None, None, None),
            P("lat", None, None),
        ),
        out_specs=P("lat", None, "groups"),
        check_vma=False,
    )
```

```python
import math

import jax
import jax.numpy as jnp
from jax import lax
from jax.experimental import pallas as pl
from jax.experimental.pallas import tpu as pltpu
from jax.sharding import PartitionSpec as P

F32, BF16, I16, I32 = jnp.float32, jnp.bfloat16, jnp.int16, jnp.int32
LANES = 128
BLOCK = 8
CODE = 32000.0


def from_partner(block, axis, distance):
    count = lax.axis_size(axis)
    route = []
    for low in range(count):
        high = low | 1 << distance
        if high != low and high < count:
            route += [(low, high), (high, low)]
    return lax.ppermute(block, axis, route)


def lanes_of(shape):
    return lax.broadcasted_iota(I32, shape, len(shape) - 1)


def cos_sin(step, nlon):
    quarter, eighth = nlon // 4, nlon // 8
    moved = step + eighth
    quadrant = moved // quarter & 3
    x = ((moved & quarter - 1) - eighth).astype(F32) * F32(2.0 * math.pi / nlon)
    y = x * x
    c = 1.0 + y * (-0.5 + y * (1 / 24 + y * (-1 / 720 + y * (1 / 40320 - y / 3628800))))
    s = x * (1.0 + y * (-1 / 6 + y * (1 / 120 + y * (-1 / 5040 + y / 362880))))
    swap = quadrant & 1 == 1
    cos = jnp.where(swap, s, c)
    sin = jnp.where(swap, c, s)
    cos = jnp.where((quadrant == 1) | (quadrant == 2), -cos, cos)
    sin = jnp.where(quadrant >= 2, -sin, sin)
    return cos, sin


def split(value):
    high = value.astype(BF16)
    return high, (value - high.astype(F32)).astype(BF16)


def encode(values, send):
    rank = values[0].shape[0]
    peak = jnp.full((8, LANES), 1e-30, F32)
    for value in values:
        for row in range(0, rank, 8):
            peak = jnp.maximum(peak, jnp.abs(value[row : row + 8]))
    exponent = jnp.ceil(jnp.log2(peak))
    scale = jnp.exp2(-exponent) * CODE
    scale = jnp.concatenate([scale] * (rank // 8), 0)
    for g, value in enumerate(values):
        send[g * rank : (g + 1) * rank, :] = (value * scale).astype(I32).astype(I16)
    send[len(values) * rank :, :] = exponent.astype(I32).astype(I16)


def pick(product, rows, share):
    product = product[:, :LANES] + product[:, LANES:]
    place = lanes_of((rows, LANES)) % BLOCK // share
    chosen = jnp.zeros((rows, LANES), F32)
    for o in range(product.shape[0] // rows):
        chosen = jnp.where(place == o, product[o * rows : (o + 1) * rows], chosen)
    return chosen


def spread(value, share):
    halves = jnp.concatenate(split(value), 1)
    place = lanes_of(halves.shape) % share
    return [halves * jnp.where(place == o, F32(1.0), F32(0.0)).astype(BF16) for o in range(share)]


def analyse_kernel(ids_hbm, weights_hbm, leaf_hbm, transfer_hbm, grid_hbm, own_ref, send_ref, first_ref,
                   ids, weights, leaf, grid, table, turned, raw, wave_c, wave_s, sems, grid_sems, *, fields, pieces, turn):
    rows, nlon = grid.shape
    orders, cycles, rank = leaf.shape
    piece = nlon // pieces
    groups = pl.cdiv(orders, BLOCK)

    def load_of(i):
        cut = (slice(None), pl.ds(pl.multiple_of(i * piece, piece), piece))
        return pltpu.make_async_copy(grid_hbm.at[cut], grid.at[cut], grid_sems.at[i])

    loads = [load_of(i) for i in range(pieces)]
    ids_load = pltpu.make_async_copy(ids_hbm, ids, sems.at[0])
    weights_load = pltpu.make_async_copy(weights_hbm, weights, sems.at[1])
    leaf_load = pltpu.make_async_copy(leaf_hbm, leaf, sems.at[2])
    first_load = pltpu.make_async_copy(transfer_hbm.at[0], first_ref, sems.at[3])
    ids_load.start()
    weights_load.start()
    leaf_load.start()
    for load in loads:
        load.start()
    first_load.start()
    half = 48
    ids_load.wait()
    row = lax.broadcasted_iota(I32, (half, LANES), 0)
    order = jnp.zeros((half, LANES), I32)
    for o in range(orders):
        order = jnp.where(row == o, ids[o], order)
    fine_c, fine_s = cos_sin(order * lanes_of((half, LANES)) & nlon - 1, nlon)
    coarse_c, coarse_s = cos_sin(order * (lanes_of((half, LANES)) * LANES) & nlon - 1, nlon)
    turn_c = coarse_c[:, turn // LANES : turn // LANES + 1] + jnp.zeros((half, LANES), F32)
    turn_s = coarse_s[:, turn // LANES : turn // LANES + 1] + jnp.zeros((half, LANES), F32)
    for a in range(turn // LANES):
        ca, sa = coarse_c[:, a : a + 1], coarse_s[:, a : a + 1]
        at = slice(a * LANES, (a + 1) * LANES)
        wave_c[:, at], wave_s[:, at] = ca * fine_c - sa * fine_s, sa * fine_c + ca * fine_s

    def fill(i, carry):
        for a in range(turn // LANES):
            at = slice(a * LANES, (a + 1) * LANES)
            to = pl.ds(pl.multiple_of(i * turn + a * LANES, LANES), LANES)
            c, s = wave_c[:, at], wave_s[:, at]
            table[0:half, to] = c.astype(BF16)
            table[64 : 64 + half, to] = (-s).astype(BF16)
            wave_c[:, at], wave_s[:, at] = c * turn_c - s * turn_s, s * turn_c + c * turn_s
        return carry

    lax.fori_loop(0, nlon // turn, fill, 0)
    weights_load.wait()
    leaf_load.wait()
    raw[:, :] = jnp.zeros(raw.shape, F32)
    share = pl.cdiv(orders // 2, pieces)
    turned[orders // 2 * rank :, :] = jnp.zeros((turned.shape[0] - orders // 2 * rank, 2 * cycles), BF16)

    def multiply(i, carry):
        load_of(i).wait()
        at = pl.ds(pl.multiple_of(i * piece, piece), piece)
        raw[:, :] += lax.dot_general(grid[:, at], table[:, at], (((1,), (1,)), ((), ())), preferred_element_type=F32)
        begin = jnp.minimum(i * share, orders // 2 - share)
        for u in range(share):
            o = begin + u
            turned[pl.ds(pl.multiple_of(o * rank, rank), rank), :] = jnp.concatenate([leaf[2 * o], leaf[2 * o + 1]], 0).T
        return carry

    lax.fori_loop(0, pieces, multiply, 0)
    weight = jnp.broadcast_to(weights[:, :], (LANES, cycles)).T * F32(1.0 / math.sqrt(nlon))
    moved = []
    for f in range(fields):
        value = raw[pl.ds(f, cycles, stride=fields), :] * weight
        moved.append(pltpu.roll(value, BLOCK * f, 1) if f else value)
    slot = lanes_of((cycles, LANES)) // BLOCK
    results = []
    for g in range(groups):
        here = slot - g & fields - 1
        waves = moved[0]
        for f in range(1, fields):
            waves = jnp.where(here == f, moved[f], waves)
        pairs = [turned[p * rank : (p + 1) * rank, :] for p in range(g * BLOCK // 2, (g + 1) * BLOCK // 2)]
        left = jnp.concatenate([jnp.concatenate(pairs[p : p + 2], 1) for p in range(0, len(pairs), 2)], 0)
        product = jnp.dot(left, jnp.concatenate(spread(waves, 4), 0), preferred_element_type=F32)
        results.append(pick(product, rank, 4))
    for g in range(groups):
        own_ref[g * rank : (g + 1) * rank, :] = results[g]
    encode(results, send_ref)
    first_load.wait()


def join(own_ref, got_ref, joined, upper, groups, rank):
    exponent = got_ref[groups * rank :, :].astype(I32).astype(F32)
    scale = jnp.exp2(exponent) * F32(1.0 / CODE)
    scale = jnp.concatenate([scale] * (rank // 8), 0)
    for g in range(groups):
        at = slice(g * rank, (g + 1) * rank)
        own = own_ref[at, :]
        other = got_ref[at, :].astype(I32).astype(F32) * scale
        for o, value in enumerate(spread(jnp.where(upper, other, own), 2)):
            joined[g, 2 * o * rank : (2 * o + 1) * rank, :] = value
        for o, value in enumerate(spread(jnp.where(upper, own, other), 2)):
            joined[g, (2 * o + 1) * rank : (2 * o + 2) * rank, :] = value


def merge(factors, joined, groups):
    orders, rank, wide = factors.shape
    results = []
    for g in range(groups):
        first = range(g * BLOCK, min((g + 1) * BLOCK, orders), 2)
        left = jnp.concatenate([jnp.concatenate([factors[o], factors[o + 1]], 1) for o in first], 0)
        product = jnp.dot(left, joined[g], preferred_element_type=F32)
        results.append(pick(product, rank, 2))
    return results


def level_kernel(own_ref, got_ref, factors_ref, next_ref, send_ref, joined, *, level):
    factors = factors_ref.at[level - 1] if level else factors_ref
    orders, rank, _ = factors.shape
    groups = joined.shape[0]
    upper = (lax.axis_index("lat") >> level) & 1 == 1
    join(own_ref, got_ref, joined, upper, groups, rank)
    results = merge(factors, joined, groups)
    for g in range(groups):
        next_ref[g * rank : (g + 1) * rank, :] = results[g]
    encode(results, send_ref)


def fetch_kernel(after_ref, ids_hbm, transfer_hbm, last_hbm, factors_ref, quads_ref, lanes_ref, ids, last_ref, sems):
    del after_ref
    ids_load = pltpu.make_async_copy(ids_hbm, ids, sems.at[0])
    factors_load = pltpu.make_async_copy(transfer_hbm.at[1:], factors_ref, sems.at[1])
    last_load = pltpu.make_async_copy(last_hbm, last_ref, sems.at[2])
    ids_load.start()
    factors_load.start()
    last_load.start()
    ids_load.wait()
    lane = lanes_of((8, LANES)) % BLOCK
    for g in range(lanes_ref.shape[0]):
        order = jnp.zeros((8, LANES), I32)
        for o in range(min(BLOCK, ids.shape[0] - g * BLOCK)):
            order = jnp.where(lane == o, ids[g * BLOCK + o], order)
        lanes_ref[g] = order
    last_load.wait()
    orders, degrees, rank = last_ref.shape
    quads_ref[orders // 4 * degrees :, :] = jnp.zeros((quads_ref.shape[0] - orders // 4 * degrees, 4 * rank), BF16)
    for o in range(0, orders, 2):
        at = slice(o // 4 * degrees, (o // 4 + 1) * degrees)
        quads_ref[at, o % 4 * rank : (o % 4 + 2) * rank] = jnp.concatenate([last_ref[o], last_ref[o + 1]], 1)
    factors_load.wait()


def last_kernel(lanes_ref, own_ref, got_ref, factors_ref, quads_ref, out_ref, joined, *, level):
    factors = factors_ref.at[level - 1]
    orders, rank, _ = factors.shape
    groups = joined.shape[0]
    degrees = quads_ref.shape[0] * 4 // (groups * BLOCK)
    slots = LANES // BLOCK
    position = lax.axis_index("lat")
    upper = (position >> level) & 1 == 1
    join(own_ref, got_ref, joined, upper, groups, rank)
    finals = merge(factors, joined, groups)
    lane = lanes_of((degrees, LANES))
    degree = position * degrees + lax.broadcasted_iota(I32, (degrees, LANES), 0)
    outs = []
    for g in range(groups):
        left = quads_ref[2 * g * degrees : 2 * (g + 1) * degrees, :]
        product = jnp.dot(left, jnp.concatenate(spread(finals[g], 4), 0), preferred_element_type=F32)
        value = pick(product, degrees, 4)
        order = jnp.concatenate([lanes_ref[g]] * (degrees // 8), 0)
        outs.append(jnp.where(degree >= order, value, F32(0.0)))
    slot = lane // BLOCK
    for q in range(slots):
        value = outs[0]
        for g in range(1, groups):
            value = jnp.where(slot == (q + g) % slots, outs[g], value)
        value = pltpu.roll(value, (LANES - BLOCK * q) % LANES, 1) if q else value
        out_ref[pl.ds(q, degrees, stride=slots), :] = value[:, :orders]


def in_vmem(value):
    return pltpu.with_memory_space_constraint(value, pltpu.VMEM)


def in_hbm(value):
    return pltpu.with_memory_space_constraint(value, pltpu.HBM)


def body(grid, cycle_weights, order_ids, leaf_weight, transfer, degree_weight):
    cycles, fields, nlon = grid.shape
    orders, rank = leaf_weight.shape[1:]
    levels = transfer.shape[0]
    degrees = degree_weight.shape[0]
    groups = -(-orders // BLOCK)
    pieces = 2
    leaf = leaf_weight.transpose(1, 0, 2)
    last = degree_weight.transpose(1, 0, 2)
    hbm = pl.BlockSpec(memory_space=pltpu.HBM)
    vmem = pl.BlockSpec(memory_space=pltpu.VMEM)
    own_type = pltpu.VMEM((groups * rank, LANES), F32)
    send_type = pltpu.VMEM((groups * rank + 8, LANES), I16)
    joined = pltpu.VMEM((groups, 4 * rank, 2 * LANES), BF16)
    own, send, first = pl.pallas_call(
        lambda *refs: analyse_kernel(*refs, fields=fields, pieces=pieces, turn=1024),
        out_shape=(own_type, send_type, pltpu.VMEM(transfer.shape[2:], BF16)),
        in_specs=[hbm] * 5,
        out_specs=(vmem,) * 3,
        scratch_shapes=[
            pltpu.SMEM((orders,), I32),
            pltpu.VMEM((1, cycles), F32),
            pltpu.VMEM((orders, cycles, rank), BF16),
            pltpu.VMEM((cycles * fields, nlon), BF16),
            pltpu.VMEM((LANES, nlon), BF16),
            pltpu.VMEM((groups * BLOCK // 2 * rank, 2 * cycles), BF16),
            pltpu.VMEM((cycles * fields, LANES), F32),
            pltpu.VMEM((48, 1024), F32),
            pltpu.VMEM((48, 1024), F32),
            pltpu.SemaphoreType.DMA((4,)),
            pltpu.SemaphoreType.DMA((pieces,)),
        ],
        compiler_params=pltpu.CompilerParams(vmem_limit_bytes=32 * 2**20),
        name="analyse",
    )(*map(in_hbm, (order_ids, cycle_weights.reshape(1, cycles), leaf, transfer[:, 0], grid.reshape(cycles * fields, nlon))))
    own, send, first = map(in_vmem, (own, send, first))
    for level in range(levels):
        got = in_vmem(from_partner(send, "lat", level))
        if level + 1 < levels:
            own, send = pl.pallas_call(
                lambda *refs, level=level: level_kernel(*refs, level=level),
                out_shape=(own_type, send_type),
                in_specs=[vmem, vmem, vmem],
                out_specs=(vmem, vmem),
                scratch_shapes=[joined],
                compiler_params=pltpu.CompilerParams(vmem_limit_bytes=16 * 2**20),
                name=f"level{level}",
            )(own, got, factors if level else first)
            own, send = in_vmem(own), in_vmem(send)
            if not level:
                factors, quads, order_lanes = map(in_vmem, pl.pallas_call(
                    fetch_kernel,
                    out_shape=(
                        pltpu.VMEM((levels - 1,) + transfer.shape[2:], BF16),
                        pltpu.VMEM((groups * 2 * degrees, 4 * rank), BF16),
                        pltpu.VMEM((groups, 8, LANES), I32),
                    ),
                    in_specs=[vmem] + [hbm] * 3,
                    out_specs=(vmem,) * 3,
                    scratch_shapes=[pltpu.SMEM((orders,), I32), pltpu.VMEM(last.shape, BF16), pltpu.SemaphoreType.DMA((3,))],
                    compiler_params=pltpu.CompilerParams(vmem_limit_bytes=16 * 2**20),
                    name="fetch",
                )(own, *map(in_hbm, (order_ids, transfer[:, 0], last))))
        else:
            out = pl.pallas_call(
                lambda *refs: last_kernel(*refs, level=level),
                out_shape=jax.ShapeDtypeStruct((degrees * 2 * fields, orders), F32),
                in_specs=[vmem] * 5,
                out_specs=vmem,
                scratch_shapes=[joined],
                compiler_params=pltpu.CompilerParams(vmem_limit_bytes=16 * 2**20),
                name="last",
            )(order_lanes, own, got, factors, quads)
    return out.reshape(degrees, 2 * fields, orders).transpose(0, 2, 1)


def solution(mesh):
    return jax.shard_map(
        body,
        mesh=mesh,
        in_specs=(
            P("lat", "groups", None),
            P("lat"),
            P(),
            P("lat", None, None),
            P(None, "lat", None, None, None),
            P("lat", None, None),
        ),
        out_specs=P("lat", None, "groups"),
        check_vma=False,
    )
```

```python
import math

import jax
import jax.numpy as jnp
from jax import lax
from jax.experimental import pallas as pl
from jax.experimental.pallas import tpu as pltpu
from jax.sharding import PartitionSpec as P

F32, BF16, I16, I32 = jnp.float32, jnp.bfloat16, jnp.int16, jnp.int32
LANES = 128
BLOCK = 8
CODE = 32000.0
SPARE = 6
FOLD = 16


def visit(groups):
    return [0, groups - 1, *range(1, groups - 1)]


def from_partner(block, axis, distance):
    count = lax.axis_size(axis)
    route = []
    for low in range(count):
        high = low | 1 << distance
        if high != low and high < count:
            route += [(low, high), (high, low)]
    return lax.ppermute(block, axis, route)


def lanes_of(shape):
    return lax.broadcasted_iota(I32, shape, len(shape) - 1)


def cos_sin(step, nlon):
    quarter, eighth = nlon // 4, nlon // 8
    moved = step + eighth
    quadrant = moved // quarter & 3
    x = ((moved & quarter - 1) - eighth).astype(F32) * F32(2.0 * math.pi / nlon)
    y = x * x
    c = 1.0 + y * (-0.5 + y * (1 / 24 + y * (-1 / 720 + y * (1 / 40320 - y / 3628800))))
    s = x * (1.0 + y * (-1 / 6 + y * (1 / 120 + y * (-1 / 5040 + y / 362880))))
    swap = quadrant & 1 == 1
    cos = jnp.where(swap, s, c)
    sin = jnp.where(swap, c, s)
    cos = jnp.where((quadrant == 1) | (quadrant == 2), -cos, cos)
    sin = jnp.where(quadrant >= 2, -sin, sin)
    return cos, sin


def split(value):
    high = value.astype(BF16)
    return high, (value - high.astype(F32)).astype(BF16)


def fold(value):
    free = lanes_of((FOLD, LANES)) % BLOCK >= SPARE
    rows = [value[row : row + FOLD] for row in range(0, value.shape[0], FOLD)]
    return jnp.concatenate([jnp.where(free, pltpu.roll(rows[0], BLOCK - 2 * k, 1), rows[k]) for k in range(1, len(rows))], 0)


def unfold(value):
    place = lanes_of((FOLD, LANES)) % BLOCK // 2
    head = value[:FOLD]
    for k in range(1, value.shape[0] // FOLD + 1):
        moved = pltpu.roll(value[(k - 1) * FOLD : k * FOLD], LANES - BLOCK + 2 * k, 1)
        head = jnp.where(place == k - 1, moved, head)
    return jnp.concatenate([head, value], 0)


def encode(values, send):
    values = [*values[:-1], fold(values[-1])]
    peak = jnp.full((8, LANES), 1e-30, F32)
    for value in values:
        for row in range(0, value.shape[0], 8):
            peak = jnp.maximum(peak, jnp.abs(value[row : row + 8]))
    exponent = jnp.ceil(jnp.log2(peak))
    scale = jnp.exp2(-exponent) * CODE
    at = 0
    for value in values:
        rows = value.shape[0]
        send[at : at + rows, :] = (value * jnp.concatenate([scale] * (rows // 8), 0)).astype(I32).astype(I16)
        at += rows
    send[at:, :] = exponent.astype(I32).astype(I16)


def pick(product, rows, share):
    product = product[:, :LANES] + product[:, LANES:]
    place = lanes_of((rows, LANES)) % BLOCK // share
    chosen = jnp.zeros((rows, LANES), F32)
    for o in range(product.shape[0] // rows):
        chosen = jnp.where(place == o, product[o * rows : (o + 1) * rows], chosen)
    return chosen


def spread(value, share):
    halves = jnp.concatenate(split(value), 1)
    place = lanes_of(halves.shape) % share
    return [halves * jnp.where(place == o, F32(1.0), F32(0.0)).astype(BF16) for o in range(share)]


def analyse_kernel(ids_hbm, weights_hbm, leaf_hbm, transfer_hbm, grid_hbm, own_ref, send_ref, first_ref,
                   ids, weights, leaf, grid, table, turned, raw, wave_c, wave_s, sems, grid_sems, *, fields, pieces, turn):
    rows, nlon = grid.shape
    orders, cycles, rank = leaf.shape
    piece = nlon // pieces
    groups = pl.cdiv(orders, BLOCK)

    def load_of(i):
        cut = (slice(None), pl.ds(pl.multiple_of(i * piece, piece), piece))
        return pltpu.make_async_copy(grid_hbm.at[cut], grid.at[cut], grid_sems.at[i])

    loads = [load_of(i) for i in range(pieces)]
    ids_load = pltpu.make_async_copy(ids_hbm, ids, sems.at[0])
    weights_load = pltpu.make_async_copy(weights_hbm, weights, sems.at[1])
    leaf_load = pltpu.make_async_copy(leaf_hbm, leaf, sems.at[2])
    first_load = pltpu.make_async_copy(transfer_hbm.at[0], first_ref, sems.at[3])
    ids_load.start()
    weights_load.start()
    leaf_load.start()
    for load in loads:
        load.start()
    first_load.start()
    half = 48
    ids_load.wait()
    row = lax.broadcasted_iota(I32, (8, LANES), 0)
    order = []
    for begin in range(0, half, 8):
        order.append(jnp.zeros((8, LANES), I32))
        for o in range(begin, min(begin + 8, orders)):
            order[-1] = jnp.where(row == o - begin, ids[o], order[-1])
    order = jnp.concatenate(order, 0)
    fine_c, fine_s = cos_sin(order * lanes_of((half, LANES)) & nlon - 1, nlon)
    coarse_c, coarse_s = cos_sin(order * (lanes_of((half, LANES)) * LANES) & nlon - 1, nlon)
    turn_c = coarse_c[:, turn // LANES : turn // LANES + 1] + jnp.zeros((half, LANES), F32)
    turn_s = coarse_s[:, turn // LANES : turn // LANES + 1] + jnp.zeros((half, LANES), F32)
    for a in range(turn // LANES):
        ca, sa = coarse_c[:, a : a + 1], coarse_s[:, a : a + 1]
        at = slice(a * LANES, (a + 1) * LANES)
        wave_c[:, at], wave_s[:, at] = ca * fine_c - sa * fine_s, -(sa * fine_c + ca * fine_s)

    def fill(a, carry):
        at = pl.ds(pl.multiple_of(a * LANES, LANES), LANES)
        c, s = wave_c[:, at], wave_s[:, at]
        for i in range(nlon // turn):
            to = pl.ds(pl.multiple_of(i * turn + a * LANES, LANES), LANES)
            table[0:half, to] = c.astype(BF16)
            table[64 : 64 + half, to] = s.astype(BF16)
            c, s = c * turn_c + s * turn_s, s * turn_c - c * turn_s
        return carry

    lax.fori_loop(0, turn // LANES, fill, 0)
    weights_load.wait()
    leaf_load.wait()
    raw[:, :] = jnp.zeros(raw.shape, F32)
    share = pl.cdiv(orders // 2, pieces)
    turned[orders // 2 * rank :, :] = jnp.zeros((turned.shape[0] - orders // 2 * rank, 2 * cycles), BF16)

    def multiply(i, carry):
        load_of(i).wait()
        at = pl.ds(pl.multiple_of(i * piece, piece), piece)
        raw[:, :] += lax.dot_general(grid[:, at], table[:, at], (((1,), (1,)), ((), ())), preferred_element_type=F32)
        begin = jnp.minimum(i * share, orders // 2 - share)
        for u in range(share):
            o = begin + u
            turned[pl.ds(pl.multiple_of(o * rank, rank), rank), :] = jnp.concatenate([leaf[2 * o], leaf[2 * o + 1]], 0).T
        return carry

    lax.fori_loop(0, pieces, multiply, 0)
    weight = jnp.broadcast_to(weights[:, :], (LANES, cycles)).T * F32(1.0 / math.sqrt(nlon))
    moved = []
    for f in range(fields):
        value = raw[pl.ds(f, cycles, stride=fields), :] * weight
        moved.append(pltpu.roll(value, BLOCK * f, 1) if f else value)
    slot = lanes_of((cycles, LANES)) // BLOCK
    results = []
    for g in range(groups):
        here = slot - g & fields - 1
        waves = moved[0]
        for f in range(1, fields):
            waves = jnp.where(here == f, moved[f], waves)
        pairs = [turned[p * rank : (p + 1) * rank, :] for p in range(g * BLOCK // 2, (g + 1) * BLOCK // 2)]
        left = jnp.concatenate([jnp.concatenate(pairs[p : p + 2], 1) for p in range(0, len(pairs), 2)], 0)
        product = jnp.dot(left, jnp.concatenate(spread(waves, 4), 0), preferred_element_type=F32)
        results.append(pick(product, rank, 4))
    for g in range(groups):
        own_ref[g * rank : (g + 1) * rank, :] = results[g]
    encode(results, send_ref)
    first_load.wait()


def join(own_ref, got_ref, joined, upper, groups, rank):
    exponent = got_ref[groups * rank - FOLD :, :].astype(I32).astype(F32)
    scale = jnp.exp2(exponent) * F32(1.0 / CODE)
    scale = jnp.concatenate([scale] * (rank // 8), 0)
    for g in visit(groups):
        at = slice(g * rank, (g + 1) * rank)
        own = own_ref[at, :]
        if g + 1 < groups:
            other = got_ref[at, :].astype(I32).astype(F32) * scale
        else:
            other = unfold(got_ref[g * rank : (g + 1) * rank - FOLD, :].astype(I32).astype(F32) * scale[FOLD:])
        for o, value in enumerate(spread(jnp.where(upper, other, own), 2)):
            joined[g, 2 * o * rank : (2 * o + 1) * rank, :] = value
        for o, value in enumerate(spread(jnp.where(upper, own, other), 2)):
            joined[g, (2 * o + 1) * rank : (2 * o + 2) * rank, :] = value


def merge(factors, joined, groups):
    orders, rank, wide = factors.shape
    results = {}
    for g in visit(groups):
        first = range(g * BLOCK, min((g + 1) * BLOCK, orders), 2)
        left = jnp.concatenate([jnp.concatenate([factors[o], factors[o + 1]], 1) for o in first], 0)
        product = jnp.dot(left, joined[g], preferred_element_type=F32)
        results[g] = pick(product, rank, 2)
    return [results[g] for g in range(groups)]


def level_kernel(own_ref, got_ref, factors_ref, next_ref, send_ref, joined, *, level):
    factors = factors_ref.at[level - 1] if level else factors_ref
    orders, rank, _ = factors.shape
    groups = joined.shape[0]
    upper = (lax.axis_index("lat") >> level) & 1 == 1
    join(own_ref, got_ref, joined, upper, groups, rank)
    results = merge(factors, joined, groups)
    for g in range(groups):
        next_ref[g * rank : (g + 1) * rank, :] = results[g]
    encode(results, send_ref)


def fetch_kernel(after_ref, ids_hbm, transfer_hbm, last_hbm, factors_ref, quads_ref, lanes_ref, ids, last_ref, sems):
    del after_ref
    ids_load = pltpu.make_async_copy(ids_hbm, ids, sems.at[0])
    factors_load = pltpu.make_async_copy(transfer_hbm.at[1:], factors_ref, sems.at[1])
    last_load = pltpu.make_async_copy(last_hbm, last_ref, sems.at[2])
    ids_load.start()
    factors_load.start()
    last_load.start()
    ids_load.wait()
    lane = lanes_of((8, LANES)) % BLOCK
    for g in range(lanes_ref.shape[0]):
        order = jnp.zeros((8, LANES), I32)
        for o in range(min(BLOCK, ids.shape[0] - g * BLOCK)):
            order = jnp.where(lane == o, ids[g * BLOCK + o], order)
        lanes_ref[g] = order
    last_load.wait()
    orders, degrees, rank = last_ref.shape
    quads_ref[orders // 4 * degrees :, :] = jnp.zeros((quads_ref.shape[0] - orders // 4 * degrees, 4 * rank), BF16)
    for o in range(0, orders, 2):
        at = slice(o // 4 * degrees, (o // 4 + 1) * degrees)
        quads_ref[at, o % 4 * rank : (o % 4 + 2) * rank] = jnp.concatenate([last_ref[o], last_ref[o + 1]], 1)
    factors_load.wait()


def last_kernel(lanes_ref, own_ref, got_ref, factors_ref, quads_ref, out_ref, joined, *, level):
    factors = factors_ref.at[level - 1]
    orders, rank, _ = factors.shape
    groups = joined.shape[0]
    degrees = quads_ref.shape[0] * 4 // (groups * BLOCK)
    slots = LANES // BLOCK
    position = lax.axis_index("lat")
    upper = (position >> level) & 1 == 1
    join(own_ref, got_ref, joined, upper, groups, rank)
    finals = merge(factors, joined, groups)
    lane = lanes_of((degrees, LANES))
    degree = position * degrees + lax.broadcasted_iota(I32, (degrees, LANES), 0)
    outs = []
    for g in range(groups):
        left = quads_ref[2 * g * degrees : 2 * (g + 1) * degrees, :]
        product = jnp.dot(left, jnp.concatenate(spread(finals[g], 4), 0), preferred_element_type=F32)
        value = pick(product, degrees, 4)
        order = jnp.concatenate([lanes_ref[g]] * (degrees // 8), 0)
        outs.append(jnp.where(degree >= order, value, F32(0.0)))
    slot = lane // BLOCK
    for q in range(slots):
        value = outs[0]
        for g in range(1, groups):
            value = jnp.where(slot == (q + g) % slots, outs[g], value)
        value = pltpu.roll(value, (LANES - BLOCK * q) % LANES, 1) if q else value
        out_ref[pl.ds(q, degrees, stride=slots), :] = value[:, :orders]


def in_vmem(value):
    return pltpu.with_memory_space_constraint(value, pltpu.VMEM)


def in_hbm(value):
    return pltpu.with_memory_space_constraint(value, pltpu.HBM)


def body(grid, cycle_weights, order_ids, leaf_weight, transfer, degree_weight):
    cycles, fields, nlon = grid.shape
    orders, rank = leaf_weight.shape[1:]
    levels = transfer.shape[0]
    degrees = degree_weight.shape[0]
    groups = -(-orders // BLOCK)
    pieces = 2
    leaf = leaf_weight.transpose(1, 0, 2)
    last = degree_weight.transpose(1, 0, 2)
    hbm = pl.BlockSpec(memory_space=pltpu.HBM)
    vmem = pl.BlockSpec(memory_space=pltpu.VMEM)
    own_type = pltpu.VMEM((groups * rank, LANES), F32)
    send_type = pltpu.VMEM((groups * rank - FOLD + 8, LANES), I16)
    joined = pltpu.VMEM((groups, 4 * rank, 2 * LANES), BF16)
    own, send, first = pl.pallas_call(
        lambda *refs: analyse_kernel(*refs, fields=fields, pieces=pieces, turn=1024),
        out_shape=(own_type, send_type, pltpu.VMEM(transfer.shape[2:], BF16)),
        in_specs=[hbm] * 5,
        out_specs=(vmem,) * 3,
        scratch_shapes=[
            pltpu.SMEM((orders,), I32),
            pltpu.VMEM((1, cycles), F32),
            pltpu.VMEM((orders, cycles, rank), BF16),
            pltpu.VMEM((cycles * fields, nlon), BF16),
            pltpu.VMEM((LANES, nlon), BF16),
            pltpu.VMEM((groups * BLOCK // 2 * rank, 2 * cycles), BF16),
            pltpu.VMEM((cycles * fields, LANES), F32),
            pltpu.VMEM((48, 1024), F32),
            pltpu.VMEM((48, 1024), F32),
            pltpu.SemaphoreType.DMA((4,)),
            pltpu.SemaphoreType.DMA((pieces,)),
        ],
        compiler_params=pltpu.CompilerParams(vmem_limit_bytes=32 * 2**20),
        name="analyse",
    )(*map(in_hbm, (order_ids, cycle_weights.reshape(1, cycles), leaf, transfer[:, 0], grid.reshape(cycles * fields, nlon))))
    own, send, first = map(in_vmem, (own, send, first))
    for level in range(levels):
        got = in_vmem(from_partner(send, "lat", level))
        if level + 1 < levels:
            own, send = pl.pallas_call(
                lambda *refs, level=level: level_kernel(*refs, level=level),
                out_shape=(own_type, send_type),
                in_specs=[vmem, vmem, vmem],
                out_specs=(vmem, vmem),
                scratch_shapes=[joined],
                compiler_params=pltpu.CompilerParams(vmem_limit_bytes=16 * 2**20),
                name=f"level{level}",
            )(own, got, factors if level else first)
            own, send = in_vmem(own), in_vmem(send)
            if not level:
                factors, quads, order_lanes = map(in_vmem, pl.pallas_call(
                    fetch_kernel,
                    out_shape=(
                        pltpu.VMEM((levels - 1,) + transfer.shape[2:], BF16),
                        pltpu.VMEM((groups * 2 * degrees, 4 * rank), BF16),
                        pltpu.VMEM((groups, 8, LANES), I32),
                    ),
                    in_specs=[vmem] + [hbm] * 3,
                    out_specs=(vmem,) * 3,
                    scratch_shapes=[pltpu.SMEM((orders,), I32), pltpu.VMEM(last.shape, BF16), pltpu.SemaphoreType.DMA((3,))],
                    compiler_params=pltpu.CompilerParams(vmem_limit_bytes=16 * 2**20),
                    name="fetch",
                )(own, *map(in_hbm, (order_ids, transfer[:, 0], last))))
        else:
            out = pl.pallas_call(
                lambda *refs: last_kernel(*refs, level=level),
                out_shape=jax.ShapeDtypeStruct((degrees * 2 * fields, orders), F32),
                in_specs=[vmem] * 5,
                out_specs=vmem,
                scratch_shapes=[joined],
                compiler_params=pltpu.CompilerParams(vmem_limit_bytes=16 * 2**20),
                name="last",
            )(order_lanes, own, got, factors, quads)
    return out.reshape(degrees, 2 * fields, orders).transpose(0, 2, 1)


def solution(mesh):
    return jax.shard_map(
        body,
        mesh=mesh,
        in_specs=(
            P("lat", "groups", None),
            P("lat"),
            P(),
            P("lat", None, None),
            P(None, "lat", None, None, None),
            P("lat", None, None),
        ),
        out_specs=P("lat", None, "groups"),
        check_vma=False,
    )
```

```python
import math

import jax
import jax.numpy as jnp
from jax import lax
from jax.experimental import pallas as pl
from jax.experimental.pallas import tpu as pltpu
from jax.sharding import PartitionSpec as P

F32, BF16, I16, I32 = jnp.float32, jnp.bfloat16, jnp.int16, jnp.int32
LANES = 128
BLOCK = 8
CODE = 32000.0
SPARE = 6
FOLD = 16


def visit(groups):
    return [0, 1, groups - 1, *range(2, groups - 1)]


def from_partner(block, axis, distance):
    count = lax.axis_size(axis)
    route = []
    for low in range(count):
        high = low | 1 << distance
        if high != low and high < count:
            route += [(low, high), (high, low)]
    return lax.ppermute(block, axis, route)


def lanes_of(shape):
    return lax.broadcasted_iota(I32, shape, len(shape) - 1)


def cos_sin(step, nlon):
    quarter, eighth = nlon // 4, nlon // 8
    moved = step + eighth
    quadrant = moved // quarter & 3
    x = ((moved & quarter - 1) - eighth).astype(F32) * F32(2.0 * math.pi / nlon)
    y = x * x
    c = 1.0 + y * (-0.5 + y * (1 / 24 + y * (-1 / 720 + y * (1 / 40320 - y / 3628800))))
    s = x * (1.0 + y * (-1 / 6 + y * (1 / 120 + y * (-1 / 5040 + y / 362880))))
    swap = quadrant & 1 == 1
    cos = jnp.where(swap, s, c)
    sin = jnp.where(swap, c, s)
    cos = jnp.where((quadrant == 1) | (quadrant == 2), -cos, cos)
    sin = jnp.where(quadrant >= 2, -sin, sin)
    return cos, sin


def split(value):
    high = value.astype(BF16)
    return high, (value - high.astype(F32)).astype(BF16)


def fold(value):
    free = lanes_of((FOLD, LANES)) % BLOCK >= SPARE
    rows = [value[row : row + FOLD] for row in range(0, value.shape[0], FOLD)]
    return jnp.concatenate([jnp.where(free, pltpu.roll(rows[0], BLOCK - 2 * k, 1), rows[k]) for k in range(1, len(rows))], 0)


def unfold(value):
    place = lanes_of((FOLD, LANES)) % BLOCK // 2
    head = value[:FOLD]
    for k in range(1, value.shape[0] // FOLD + 1):
        moved = pltpu.roll(value[(k - 1) * FOLD : k * FOLD], LANES - BLOCK + 2 * k, 1)
        head = jnp.where(place == k - 1, moved, head)
    return jnp.concatenate([head, value], 0)


def encode(values, send):
    values = [*values[:-1], fold(values[-1])]
    peak = jnp.full((8, LANES), 1e-30, F32)
    for value in values:
        for row in range(0, value.shape[0], 8):
            peak = jnp.maximum(peak, jnp.abs(value[row : row + 8]))
    exponent = jnp.ceil(jnp.log2(peak))
    scale = jnp.exp2(-exponent) * CODE
    at = 0
    for value in values:
        rows = value.shape[0]
        send[at : at + rows, :] = (value * jnp.concatenate([scale] * (rows // 8), 0)).astype(I32).astype(I16)
        at += rows
    send[at:, :] = exponent.astype(I32).astype(I16)


def pick(product, rows, share):
    product = product[:, :LANES] + product[:, LANES:]
    place = lanes_of((rows, LANES)) % BLOCK // share
    chosen = jnp.zeros((rows, LANES), F32)
    for o in range(product.shape[0] // rows):
        chosen = jnp.where(place == o, product[o * rows : (o + 1) * rows], chosen)
    return chosen


def spread(value, share):
    halves = jnp.concatenate(split(value), 1)
    place = lanes_of(halves.shape) % share
    return [halves * jnp.where(place == o, F32(1.0), F32(0.0)).astype(BF16) for o in range(share)]


def analyse_kernel(ids_hbm, weights_hbm, leaf_hbm, transfer_hbm, grid_hbm, own_ref, send_ref, first_ref,
                   ids, weights, leaf, grid, table, turned, raw, wave_c, wave_s, sems, grid_sems, *, fields, pieces, turn):
    rows, nlon = grid.shape
    orders, cycles, rank = leaf.shape
    piece = nlon // pieces
    groups = pl.cdiv(orders, BLOCK)

    def load_of(i):
        cut = (slice(None), pl.ds(pl.multiple_of(i * piece, piece), piece))
        return pltpu.make_async_copy(grid_hbm.at[cut], grid.at[cut], grid_sems.at[i])

    loads = [load_of(i) for i in range(pieces)]
    ids_load = pltpu.make_async_copy(ids_hbm, ids, sems.at[0])
    weights_load = pltpu.make_async_copy(weights_hbm, weights, sems.at[1])
    leaf_load = pltpu.make_async_copy(leaf_hbm, leaf, sems.at[2])
    first_load = pltpu.make_async_copy(transfer_hbm.at[0], first_ref, sems.at[3])
    ids_load.start()
    weights_load.start()
    leaf_load.start()
    for load in loads:
        load.start()
    first_load.start()
    half = 48
    ids_load.wait()
    row = lax.broadcasted_iota(I32, (8, LANES), 0)
    order = []
    for begin in range(0, half, 8):
        order.append(jnp.zeros((8, LANES), I32))
        for o in range(begin, min(begin + 8, orders)):
            order[-1] = jnp.where(row == o - begin, ids[o], order[-1])
    order = jnp.concatenate(order, 0)
    fine_c, fine_s = cos_sin(order * lanes_of((half, LANES)) & nlon - 1, nlon)
    coarse_c, coarse_s = cos_sin(order * (lanes_of((half, LANES)) * LANES) & nlon - 1, nlon)
    turn_c = coarse_c[:, turn // LANES : turn // LANES + 1] + jnp.zeros((half, LANES), F32)
    turn_s = coarse_s[:, turn // LANES : turn // LANES + 1] + jnp.zeros((half, LANES), F32)
    for a in range(turn // LANES):
        ca, sa = coarse_c[:, a : a + 1], coarse_s[:, a : a + 1]
        at = slice(a * LANES, (a + 1) * LANES)
        wave_c[:, at], wave_s[:, at] = ca * fine_c - sa * fine_s, -(sa * fine_c + ca * fine_s)

    def fill(a, carry):
        at = pl.ds(pl.multiple_of(a * LANES, LANES), LANES)
        c, s = wave_c[:, at], wave_s[:, at]
        for i in range(nlon // turn):
            to = pl.ds(pl.multiple_of(i * turn + a * LANES, LANES), LANES)
            table[0:half, to] = c.astype(BF16)
            table[64 : 64 + half, to] = s.astype(BF16)
            c, s = c * turn_c + s * turn_s, s * turn_c - c * turn_s
        return carry

    lax.fori_loop(0, turn // LANES, fill, 0)
    weights_load.wait()
    leaf_load.wait()
    raw[:, :] = jnp.zeros(raw.shape, F32)
    share = pl.cdiv(orders // 2, pieces)
    turned[orders // 2 * rank :, :] = jnp.zeros((turned.shape[0] - orders // 2 * rank, 2 * cycles), BF16)

    def multiply(i, carry):
        load_of(i).wait()
        at = pl.ds(pl.multiple_of(i * piece, piece), piece)
        raw[:, :] += lax.dot_general(grid[:, at], table[:, at], (((1,), (1,)), ((), ())), preferred_element_type=F32)
        begin = jnp.minimum(i * share, orders // 2 - share)
        for u in range(share):
            o = begin + u
            turned[pl.ds(pl.multiple_of(o * rank, rank), rank), :] = jnp.concatenate([leaf[2 * o], leaf[2 * o + 1]], 0).T
        return carry

    lax.fori_loop(0, pieces, multiply, 0)
    weight = jnp.broadcast_to(weights[:, :], (LANES, cycles)).T * F32(1.0 / math.sqrt(nlon))
    moved = []
    for f in range(fields):
        value = raw[pl.ds(f, cycles, stride=fields), :] * weight
        moved.append(pltpu.roll(value, BLOCK * f, 1) if f else value)
    slot = lanes_of((cycles, LANES)) // BLOCK
    results = []
    for g in range(groups):
        here = slot - g & fields - 1
        waves = moved[0]
        for f in range(1, fields):
            waves = jnp.where(here == f, moved[f], waves)
        pairs = [turned[p * rank : (p + 1) * rank, :] for p in range(g * BLOCK // 2, (g + 1) * BLOCK // 2)]
        left = jnp.concatenate([jnp.concatenate(pairs[p : p + 2], 1) for p in range(0, len(pairs), 2)], 0)
        product = jnp.dot(left, jnp.concatenate(spread(waves, 4), 0), preferred_element_type=F32)
        results.append(pick(product, rank, 4))
    for g in range(groups):
        own_ref[g * rank : (g + 1) * rank, :] = results[g]
    encode(results, send_ref)
    first_load.wait()


def join(own_ref, got_ref, joined, upper, groups, rank):
    exponent = got_ref[groups * rank - FOLD :, :].astype(I32).astype(F32)
    scale = jnp.exp2(exponent) * F32(1.0 / CODE)
    scale = jnp.concatenate([scale] * (rank // 8), 0)
    for g in visit(groups):
        at = slice(g * rank, (g + 1) * rank)
        own = own_ref[at, :]
        if g + 1 < groups:
            other = got_ref[at, :].astype(I32).astype(F32) * scale
        else:
            other = unfold(got_ref[g * rank : (g + 1) * rank - FOLD, :].astype(I32).astype(F32) * scale[FOLD:])
        for o, value in enumerate(spread(jnp.where(upper, other, own), 2)):
            joined[g, 2 * o * rank : (2 * o + 1) * rank, :] = value
        for o, value in enumerate(spread(jnp.where(upper, own, other), 2)):
            joined[g, (2 * o + 1) * rank : (2 * o + 2) * rank, :] = value


def merge(factors, joined, groups):
    orders, rank, wide = factors.shape
    results = {}
    for g in visit(groups):
        first = range(g * BLOCK, min((g + 1) * BLOCK, orders), 2)
        left = jnp.concatenate([jnp.concatenate([factors[o], factors[o + 1]], 1) for o in first], 0)
        product = jnp.dot(left, joined[g], preferred_element_type=F32)
        results[g] = pick(product, rank, 2)
    return [results[g] for g in range(groups)]


def level_kernel(own_ref, got_ref, factors_ref, next_ref, send_ref, joined, *, level):
    factors = factors_ref.at[level - 1] if level else factors_ref
    orders, rank, _ = factors.shape
    groups = joined.shape[0]
    upper = (lax.axis_index("lat") >> level) & 1 == 1
    join(own_ref, got_ref, joined, upper, groups, rank)
    results = merge(factors, joined, groups)
    for g in range(groups):
        next_ref[g * rank : (g + 1) * rank, :] = results[g]
    encode(results, send_ref)


def fetch_kernel(after_ref, ids_hbm, transfer_hbm, last_hbm, factors_ref, quads_ref, lanes_ref, ids, last_ref, sems):
    del after_ref
    ids_load = pltpu.make_async_copy(ids_hbm, ids, sems.at[0])
    factors_load = pltpu.make_async_copy(transfer_hbm.at[1:], factors_ref, sems.at[1])
    last_load = pltpu.make_async_copy(last_hbm, last_ref, sems.at[2])
    ids_load.start()
    factors_load.start()
    last_load.start()
    ids_load.wait()
    lane = lanes_of((8, LANES)) % BLOCK
    for g in range(lanes_ref.shape[0]):
        order = jnp.zeros((8, LANES), I32)
        for o in range(min(BLOCK, ids.shape[0] - g * BLOCK)):
            order = jnp.where(lane == o, ids[g * BLOCK + o], order)
        lanes_ref[g] = order
    last_load.wait()
    orders, degrees, rank = last_ref.shape
    quads_ref[orders // 4 * degrees :, :] = jnp.zeros((quads_ref.shape[0] - orders // 4 * degrees, 4 * rank), BF16)
    for o in range(0, orders, 2):
        at = slice(o // 4 * degrees, (o // 4 + 1) * degrees)
        quads_ref[at, o % 4 * rank : (o % 4 + 2) * rank] = jnp.concatenate([last_ref[o], last_ref[o + 1]], 1)
    factors_load.wait()


def last_kernel(lanes_ref, own_ref, got_ref, factors_ref, quads_ref, out_ref, joined, *, level):
    factors = factors_ref.at[level - 1]
    orders, rank, _ = factors.shape
    groups = joined.shape[0]
    degrees = quads_ref.shape[0] * 4 // (groups * BLOCK)
    slots = LANES // BLOCK
    position = lax.axis_index("lat")
    upper = (position >> level) & 1 == 1
    join(own_ref, got_ref, joined, upper, groups, rank)
    finals = merge(factors, joined, groups)
    lane = lanes_of((degrees, LANES))
    degree = position * degrees + lax.broadcasted_iota(I32, (degrees, LANES), 0)
    outs = []
    for g in range(groups):
        left = quads_ref[2 * g * degrees : 2 * (g + 1) * degrees, :]
        product = jnp.dot(left, jnp.concatenate(spread(finals[g], 4), 0), preferred_element_type=F32)
        value = pick(product, degrees, 4)
        order = jnp.concatenate([lanes_ref[g]] * (degrees // 8), 0)
        outs.append(jnp.where(degree >= order, value, F32(0.0)))
    slot = lane // BLOCK
    for q in range(slots):
        value = outs[0]
        for g in range(1, groups):
            value = jnp.where(slot == (q + g) % slots, outs[g], value)
        value = pltpu.roll(value, (LANES - BLOCK * q) % LANES, 1) if q else value
        out_ref[pl.ds(q, degrees, stride=slots), :] = value[:, :orders]


def in_vmem(value):
    return pltpu.with_memory_space_constraint(value, pltpu.VMEM)


def in_hbm(value):
    return pltpu.with_memory_space_constraint(value, pltpu.HBM)


def body(grid, cycle_weights, order_ids, leaf_weight, transfer, degree_weight):
    cycles, fields, nlon = grid.shape
    orders, rank = leaf_weight.shape[1:]
    levels = transfer.shape[0]
    degrees = degree_weight.shape[0]
    groups = -(-orders // BLOCK)
    pieces = 2
    leaf = leaf_weight.transpose(1, 0, 2)
    last = degree_weight.transpose(1, 0, 2)
    hbm = pl.BlockSpec(memory_space=pltpu.HBM)
    vmem = pl.BlockSpec(memory_space=pltpu.VMEM)
    own_type = pltpu.VMEM((groups * rank, LANES), F32)
    send_type = pltpu.VMEM((groups * rank - FOLD + 8, LANES), I16)
    joined = pltpu.VMEM((groups, 4 * rank, 2 * LANES), BF16)
    own, send, first = pl.pallas_call(
        lambda *refs: analyse_kernel(*refs, fields=fields, pieces=pieces, turn=1024),
        out_shape=(own_type, send_type, pltpu.VMEM(transfer.shape[2:], BF16)),
        in_specs=[hbm] * 5,
        out_specs=(vmem,) * 3,
        scratch_shapes=[
            pltpu.SMEM((orders,), I32),
            pltpu.VMEM((1, cycles), F32),
            pltpu.VMEM((orders, cycles, rank), BF16),
            pltpu.VMEM((cycles * fields, nlon), BF16),
            pltpu.VMEM((LANES, nlon), BF16),
            pltpu.VMEM((groups * BLOCK // 2 * rank, 2 * cycles), BF16),
            pltpu.VMEM((cycles * fields, LANES), F32),
            pltpu.VMEM((48, 1024), F32),
            pltpu.VMEM((48, 1024), F32),
            pltpu.SemaphoreType.DMA((4,)),
            pltpu.SemaphoreType.DMA((pieces,)),
        ],
        compiler_params=pltpu.CompilerParams(vmem_limit_bytes=32 * 2**20),
        name="analyse",
    )(*map(in_hbm, (order_ids, cycle_weights.reshape(1, cycles), leaf, transfer[:, 0], grid.reshape(cycles * fields, nlon))))
    own, send, first = map(in_vmem, (own, send, first))
    for level in range(levels):
        got = in_vmem(from_partner(send, "lat", level))
        if level + 1 < levels:
            own, send = pl.pallas_call(
                lambda *refs, level=level: level_kernel(*refs, level=level),
                out_shape=(own_type, send_type),
                in_specs=[vmem, vmem, vmem],
                out_specs=(vmem, vmem),
                scratch_shapes=[joined],
                compiler_params=pltpu.CompilerParams(vmem_limit_bytes=16 * 2**20),
                name=f"level{level}",
            )(own, got, factors if level else first)
            own, send = in_vmem(own), in_vmem(send)
            if not level:
                factors, quads, order_lanes = map(in_vmem, pl.pallas_call(
                    fetch_kernel,
                    out_shape=(
                        pltpu.VMEM((levels - 1,) + transfer.shape[2:], BF16),
                        pltpu.VMEM((groups * 2 * degrees, 4 * rank), BF16),
                        pltpu.VMEM((groups, 8, LANES), I32),
                    ),
                    in_specs=[vmem] + [hbm] * 3,
                    out_specs=(vmem,) * 3,
                    scratch_shapes=[pltpu.SMEM((orders,), I32), pltpu.VMEM(last.shape, BF16), pltpu.SemaphoreType.DMA((3,))],
                    compiler_params=pltpu.CompilerParams(vmem_limit_bytes=16 * 2**20),
                    name="fetch",
                )(own, *map(in_hbm, (order_ids, transfer[:, 0], last))))
        else:
            out = pl.pallas_call(
                lambda *refs: last_kernel(*refs, level=level),
                out_shape=jax.ShapeDtypeStruct((degrees * 2 * fields, orders), F32),
                in_specs=[vmem] * 5,
                out_specs=vmem,
                scratch_shapes=[joined],
                compiler_params=pltpu.CompilerParams(vmem_limit_bytes=16 * 2**20),
                name="last",
            )(order_lanes, own, got, factors, quads)
    return out.reshape(degrees, 2 * fields, orders).transpose(0, 2, 1)


def solution(mesh):
    return jax.shard_map(
        body,
        mesh=mesh,
        in_specs=(
            P("lat", "groups", None),
            P("lat"),
            P(),
            P("lat", None, None),
            P(None, "lat", None, None, None),
            P("lat", None, None),
        ),
        out_specs=P("lat", None, "groups"),
        check_vma=False,
    )
```
